128 devices in a mesh: data: 128 (over z, y, x, core).
Axes of the slice: x: 4, y: 4, z: 4, core: 2. Of those that a mesh axis runs over, the one named last changes fastest.
Arguments:
- tokens: bfloat16 [262144, 512], P('data')
- w_in: bfloat16 [512, 2048], replicated
- w_out: bfloat16 [2048, 512], replicated
- task_heads: bfloat16 [6, 512, 3], replicated
- labels: int32 [6, 262144], P(None, 'data')
- label_mask: int32 [6, 262144], P(None, 'data')
Outputs:
- output 1: float32 [6], replicated
- output 2: float32 [1048576], P('data')
- output 3: float32 [1048576], P('data')
All inputs are finite; a program needn't handle non-finite values.
Results may differ from the reference program's by a relative error of at most 0.00315927.
Values are sent between devices in bfloat16 or wider.
A program may use at most 1 GiB of HBM per device.

```python
import jax
import jax.numpy as jnp
from jax import lax

MODEL_DIM = 512
HIDDEN_DIM = 2048
NUM_TASKS = 6
NUM_CLASSES = 3
TOK_DEV = 2048
GROUP_SIZE = 128
SOLVER_STEPS = 20


def draw_labels(rng_key):
    sub_keys = jax.random.split(rng_key, 7)
    tokens_total = TOK_DEV * GROUP_SIZE
    dev_class = jax.random.randint(sub_keys[0], (GROUP_SIZE, 1), 0, NUM_CLASSES)
    keep_draw = jax.random.randint(sub_keys[1], (GROUP_SIZE, TOK_DEV), 0, 4)
    free_class = jax.random.randint(sub_keys[2], (GROUP_SIZE, TOK_DEV), 0, NUM_CLASSES)
    common_class = jnp.where(keep_draw < 3, dev_class, free_class).reshape(tokens_total)
    noise_draw = jax.random.randint(sub_keys[3], (NUM_TASKS, tokens_total), 0, 4)
    task_class = jax.random.randint(sub_keys[4], (NUM_TASKS, tokens_total), 0, NUM_CLASSES)
    labels = jnp.where(noise_draw == 0, task_class, common_class[None, :]).astype(jnp.int32)
    mask_level = jax.random.randint(sub_keys[5], (NUM_TASKS, GROUP_SIZE, 1), 5, 100)
    mask_draw = jax.random.randint(sub_keys[6], (NUM_TASKS, GROUP_SIZE, TOK_DEV), 0, 100)
    label_mask = (mask_draw < mask_level).astype(jnp.int32).reshape(NUM_TASKS, tokens_total)
    return labels, label_mask


def setup_inputs(seed: int = 0) -> dict:
    rng_keys = jax.random.split(jax.random.key(seed), 6)
    tokens_total = TOK_DEV * GROUP_SIZE
    tokens = jax.random.normal(rng_keys[0], (tokens_total, MODEL_DIM), jnp.float32)
    w_in = jax.random.normal(rng_keys[1], (MODEL_DIM, HIDDEN_DIM), jnp.float32) * MODEL_DIM ** -0.5
    w_out = jax.random.normal(rng_keys[2], (HIDDEN_DIM, MODEL_DIM), jnp.float32) * HIDDEN_DIM ** -0.5
    shared_head = jax.random.normal(rng_keys[3], (MODEL_DIM, NUM_CLASSES), jnp.float32)
    own_head = jax.random.normal(rng_keys[4], (NUM_TASKS, MODEL_DIM, NUM_CLASSES), jnp.float32)
    head_sign = (1 - 2 * (jnp.arange(NUM_TASKS) % 2)).astype(jnp.float32)
    task_heads = (head_sign[:, None, None] * shared_head[None] + 0.6 * own_head) * (1.5 * MODEL_DIM ** -0.5)
    labels, label_mask = draw_labels(rng_keys[5])
    return {"tokens": tokens.astype(jnp.bfloat16), "w_in": w_in.astype(jnp.bfloat16), "w_out": w_out.astype(jnp.bfloat16), "task_heads": task_heads.astype(jnp.bfloat16), "labels": labels, "label_mask": label_mask}


def device_grads(x_loc, w_in, w_out, task_heads, lab_loc, mask_loc):
    pre_act = jnp.dot(x_loc, w_in, preferred_element_type=jnp.float32)
    act_out, gelu_slope = jax.jvp(jax.nn.gelu, (pre_act,), (jnp.ones_like(pre_act),))
    act_bf = act_out.astype(jnp.bfloat16)
    residual = x_loc.astype(jnp.float32) + jnp.dot(act_bf, w_out, preferred_element_type=jnp.float32)
    z_bf = residual.astype(jnp.bfloat16)
    heads_wide = task_heads.astype(jnp.float32)
    logits = jnp.einsum("bd,tdc->tbc", z_bf.astype(jnp.float32), heads_wide)
    soft_prob = jax.nn.softmax(logits, axis=-1)
    onehot = (lab_loc[:, :, None] == jnp.arange(NUM_CLASSES)[None, None, :]).astype(jnp.float32)
    d_logit = (mask_loc[:, :, None].astype(jnp.float32) * (soft_prob - onehot)).astype(jnp.bfloat16)
    d_resid = jnp.einsum("tbc,tdc->tbd", d_logit.astype(jnp.float32), heads_wide).astype(jnp.bfloat16)
    d_wide = d_resid.astype(jnp.float32)
    grad_w_out = jnp.einsum("bf,tbd->tfd", act_bf.astype(jnp.float32), d_wide)
    d_act = jnp.einsum("tbd,fd->tbf", d_wide, w_out.astype(jnp.float32))
    d_pre = (d_act * gelu_slope[None]).astype(jnp.bfloat16)
    grad_w_in = jnp.einsum("bd,tbf->tdf", x_loc.astype(jnp.float32), d_pre.astype(jnp.float32))
    return grad_w_in, grad_w_out


def solve_weights(gram_mat):
    step_scale = jnp.trace(gram_mat) / NUM_TASKS

    def solver_step(step_idx, weights):
        pull_vec = (gram_mat * weights[None, :]).sum(axis=1)
        raised = weights * jnp.exp(-pull_vec / step_scale)
        return raised / raised.sum()

    init_weights = jnp.full((NUM_TASKS,), 1.0 / NUM_TASKS, jnp.float32)
    return lax.fori_loop(0, SOLVER_STEPS, solver_step, init_weights)


def reference(tokens, w_in, w_out, task_heads, labels, label_mask):
    inv_count = 1.0 / jnp.maximum(label_mask.sum(axis=1), 1).astype(jnp.float32)
    tok_blocks = tokens.reshape(GROUP_SIZE, TOK_DEV, MODEL_DIM)
    lab_blocks = labels.reshape(NUM_TASKS, GROUP_SIZE, TOK_DEV).transpose(1, 0, 2)
    mask_blocks = label_mask.reshape(NUM_TASKS, GROUP_SIZE, TOK_DEV).transpose(1, 0, 2)
    flat_len = MODEL_DIM * HIDDEN_DIM

    def add_device(grad_sum, block_in):
        x_loc, lab_loc, mask_loc = block_in
        grad_w_in, grad_w_out = device_grads(x_loc, w_in, w_out, task_heads, lab_loc, mask_loc)
        flat_grad = jnp.concatenate([grad_w_in.reshape(NUM_TASKS, flat_len), grad_w_out.reshape(NUM_TASKS, flat_len)], axis=1)
        part_grad = (flat_grad * inv_count[:, None]).astype(jnp.bfloat16).astype(jnp.float32)
        return grad_sum + part_grad, None

    grad_sum, _ = lax.scan(add_device, jnp.zeros((NUM_TASKS, 2 * flat_len), jnp.float32), (tok_blocks, lab_blocks, mask_blocks))
    gram_mat = jnp.dot(grad_sum, grad_sum.T, preferred_element_type=jnp.float32)
    weights = solve_weights(gram_mat)
    combined = (weights[:, None] * grad_sum).sum(axis=0)
    return weights, combined[:flat_len], combined[flat_len:]
```

```python
import functools

import jax
import jax.numpy as jnp
from jax import lax
from jax.experimental import pallas as pl
from jax.experimental.pallas import tpu as pltpu
from jax.sharding import PartitionSpec as P

SOLVER_STEPS = 20
T = 6
MESH = pl.DeviceIdType.MESH
STRIDES = (32, 8, 2)
RING, DEPTH, XRING = 8, 4, 3
F32, BF16 = jnp.float32, jnp.bfloat16


def perm(order, z, y, x):
    return ((z, y, x), (y, x, z), (x, z, y))[order]


def kernel(rb_count, cnt_ref, aT_hbm, xT_hbm, dz_hbm, w2T_hbm, gp_hbm,
           alpha_ref, out1_ref, out2_ref,
           aT, xT, dz, w2T, gp, q, inv, hb, xr, dbuf, ebuf, fbuf, r1, r2, r3, shard, gb, ar_s, ar_r,
           ld_sem, gp_sem, xs_sem, xr_sem, s_sem, r_sem, ars_sem, arr_sem, gs_sem, gr_sem):
    nchunk = 4 * rb_count
    nfb = 2 * rb_count
    me = lax.axis_index("data")
    core = lax.rem(me, 2)
    coord = (lax.div(me, 32), lax.rem(lax.div(me, 8), 4), lax.rem(lax.div(me, 2), 4))
    partner = me + 1 - 2 * core

    def nb(dim, step):
        u = coord[dim]
        return (me + (lax.rem(u + step + 4, 4) - u) * STRIDES[dim],)

    def rel(dim, step):
        return lax.rem(coord[dim] + step + 4, 4)

    loads = [pltpu.make_async_copy(aT_hbm.at[i], aT.at[i], ld_sem.at[i]) for i in range(rb_count)]
    dz_loads = [pltpu.make_async_copy(dz_hbm.at[t], dz.at[t], ld_sem.at[rb_count + t]) for t in range(T)]
    x_load = pltpu.make_async_copy(xT_hbm, xT, ld_sem.at[rb_count + T])
    w_load = pltpu.make_async_copy(w2T_hbm, w2T, ld_sem.at[rb_count + T + 1])

    def gp_load(fb):
        cols = pl.ds(pl.multiple_of(fb * 256, 256), 256)
        return pltpu.make_async_copy(gp_hbm.at[:, cols], gp.at[lax.rem(fb, 2)], gp_sem.at[lax.rem(fb, 2)])

    loads[0].start()
    for c in dz_loads:
        c.start()
    w_load.start()
    x_load.start()
    gp_load(0).start()
    for c in loads[1:]:
        c.start()

    barrier = pltpu.get_barrier_semaphore()
    peers = [(partner,)] + [nb(d, s) for d in range(3) for s in (1, -1)]
    for p in peers:
        pl.semaphore_signal(barrier, inc=1, device_id=p, device_id_type=MESH)
    pl.semaphore_wait(barrier, 7)

    def all_reduce(base, val):
        plist = [(partner,)]
        for d in range(3):
            odd = lax.rem(coord[d], 2)
            plist.append(nb(d, 1 - 2 * odd))
            plist.append(nb(d, 2 * odd - 1))
        for i, p in enumerate(plist):
            s = base + i
            ar_s[s] = val
            cp = pltpu.make_async_remote_copy(
                src_ref=ar_s.at[s], dst_ref=ar_r.at[s], send_sem=ars_sem.at[s], recv_sem=arr_sem.at[s],
                device_id=p, device_id_type=MESH)
            cp.start()
            cp.wait()
            val = val + ar_r[s]
        return val

    total = all_reduce(0, cnt_ref[...])
    inv_all = 1.0 / jnp.maximum(total, 1.0)
    for t in range(T):
        inv[t] = jnp.broadcast_to(inv_all[t:t + 1, :], (8, 128))

    srcs = (dbuf, ebuf, fbuf)
    recvs = (r1, r2, r3)

    def dims_of(p, t):
        return (t % 3 + p) % 3, (1 if t < 3 else -1)

    def drain_sends(p, d):
        ref = recvs[p].at[0]
        pltpu.make_async_copy(ref, ref, s_sem.at[p, d]).wait()

    def send(p, k, t, blk, kind, step, dim):
        slot, d = lax.rem(k, RING), lax.rem(k, DEPTH)
        pltpu.make_async_remote_copy(
            src_ref=srcs[p].at[d, t, blk], dst_ref=recvs[p].at[slot, kind, t],
            send_sem=s_sem.at[p, d], recv_sem=r_sem.at[p, 0 if kind == 0 else 1, slot],
            device_id=nb(dim, step), device_id_type=MESH).start()

    def open_phase(p, k):
        for t in range(T):
            dim, sg = dims_of(p, t)
            send(p, k, t, rel(dim, 2), 0, sg, dim)
        for t in range(T):
            dim, sg = dims_of(p, t)
            send(p, k, t, rel(dim, -sg), 1, -sg, dim)

    def relay(p, k):
        slot, d = lax.rem(k, RING), lax.rem(k, DEPTH)
        ref = recvs[p].at[slot, 0]
        pltpu.make_async_copy(ref, ref, r_sem.at[p, 0, slot]).wait()
        for t in range(T):
            dim, sg = dims_of(p, t)
            v = rel(dim, sg)
            srcs[p][d, t, v] = srcs[p][d, t, v] + recvs[p][slot, 0, t]
        for t in range(T):
            dim, sg = dims_of(p, t)
            send(p, k, t, rel(dim, sg), 2, sg, dim)

    def close(p, k):
        slot, d = lax.rem(k, RING), lax.rem(k, DEPTH)
        ref = recvs[p].at[slot, pl.ds(1, 2)]
        pltpu.make_async_copy(ref, ref, r_sem.at[p, 1, slot]).wait()
        if p < 2:
            @pl.when(k >= DEPTH)
            def _():
                drain_sends(p + 1, d)
        for t in range(T):
            dim, _ = dims_of(p, t)
            out = srcs[p][d, t, coord[dim]] + recvs[p][slot, 1, t] + recvs[p][slot, 2, t]
            if p < 2:
                srcs[p + 1][d, t] = out
            else:
                shard[t, k] = out
        if p < 2:
            open_phase(p + 1, k)

    def half_copy(k, half):
        hs, xs = lax.rem(k, 2), lax.rem(k, XRING)
        return pltpu.make_async_remote_copy(
            src_ref=hb.at[hs, 1 - core, pl.ds(3 * half, 3)], dst_ref=xr.at[xs, pl.ds(3 * half, 3)],
            send_sem=xs_sem.at[hs, half], recv_sem=xr_sem.at[xs, half],
            device_id=(partner,), device_id_type=MESH)

    def merge(k):
        d, hs, xs = lax.rem(k, DEPTH), lax.rem(k, 2), lax.rem(k, XRING)
        half_copy(k, 0).wait_recv()
        half_copy(k, 1).wait_recv()

        @pl.when(k >= DEPTH)
        def _():
            drain_sends(0, d)
        for t in range(T):
            for pair in range(32):
                rows = slice(16 * pair, 16 * pair + 16)
                s = hb[hs, core, t, rows, :].astype(F32) + xr[xs, t, rows, :].astype(F32)
                for e in range(2):
                    i = 2 * pair + e
                    a, b, c = perm(t % 3, i // 16, (i // 4) % 4, i % 4)
                    dbuf[d, t, a, b, c] = s[8 * e:8 * e + 8]
        open_phase(0, k)

    def emit(hs, t, acc):
        row = inv[t][0:1, :]
        hb[hs, 0, t] = (acc[:, :128] * row).astype(BF16)
        hb[hs, 1, t] = (acc[:, 128:] * row).astype(BF16)

    def compute_out(k, half):
        j = lax.div(k, 2)
        rb, cb = lax.div(j, 2), lax.rem(j, 2)
        hs = lax.rem(k, 2)
        cols = pl.ds(pl.multiple_of(cb * 256, 256), 256)
        if half == 0:
            for i in range(rb_count):
                @pl.when(j == 2 * i)
                def _():
                    loads[i].wait()

        @pl.when(k == 0)
        def _():
            for t in range(3):
                dz_loads[3 * half + t].wait()

        def task(t, _):
            acc = jnp.dot(aT[rb], dz[t, :, cols], preferred_element_type=F32)
            emit(hs, t, acc)
            return 0
        lax.fori_loop(3 * half, 3 * half + 3, task, 0)

    def compute_in(k, half):
        fb = lax.div(k, 2)
        hs, gs = lax.rem(k, 2), lax.rem(fb, 2)
        if half == 0:
            @pl.when(k == 1)
            def _():
                w_load.wait()
                x_load.wait()
            gp_load(fb).wait()

            @pl.when(fb + 1 < nfb)
            def _():
                gp_load(fb + 1).start()
        tok = q.shape[0]
        step = tok // 4

        def task(t, _):
            def tile(i, _):
                rows = pl.ds(pl.multiple_of(i * step, step), step)
                d_act = jnp.dot(dz[t, rows, :], w2T[fb], preferred_element_type=F32)
                q[rows, :] = (d_act * gp[gs, rows, :]).astype(BF16)
                return 0
            lax.fori_loop(0, 4, tile, 0)
            acc = jnp.dot(xT[...], q[...], preferred_element_type=F32)
            emit(hs, t, acc)
            return 0
        lax.fori_loop(3 * half, 3 * half + 3, task, 0)

    def compute(k, half):
        @pl.when(k < nchunk)
        def _():
            if half == 0:
                @pl.when(k >= 2)
                def _():
                    half_copy(k, 0).wait_send()
                    half_copy(k, 1).wait_send()

            @pl.when(lax.rem(k, 2) == 0)
            def _():
                compute_out(k, half)

            @pl.when(lax.rem(k, 2) == 1)
            def _():
                compute_in(k, half)
            half_copy(k, half).start()

    def at(k, fn):
        @pl.when((k >= 0) & (k < nchunk))
        def _():
            fn(k)

    def slot(kk, _):
        at(kk - 3, functools.partial(relay, 0))
        at(kk - 6, functools.partial(relay, 1))
        at(kk - 9, functools.partial(relay, 2))
        compute(kk, 0)
        at(kk - 1, merge)
        at(kk - 4, functools.partial(close, 0))
        at(kk - 7, functools.partial(close, 1))
        at(kk - 10, functools.partial(close, 2))
        compute(kk, 1)
        return 0
    lax.fori_loop(0, nchunk + 10, slot, 0)

    for i in range(DEPTH):
        for p in range(3):
            drain_sends(p, i)
    for k in (nchunk - 2, nchunk - 1):
        half_copy(k, 0).wait_send()
        half_copy(k, 1).wait_send()

    pairs = [(t, s) for t in range(T) for s in range(t, T)]

    def gram_step(k, accs):
        rows = [shard[t, k] for t in range(T)]
        return tuple(acc + rows[t] * rows[s] for acc, (t, s) in zip(accs, pairs))
    accs = lax.fori_loop(0, nchunk, gram_step, tuple(jnp.zeros((8, 128), F32) for _ in pairs))
    row_id = lax.broadcasted_iota(jnp.int32, (8, 128), 0)
    col_id = lax.broadcasted_iota(jnp.int32, (8, 128), 1)
    gram = jnp.zeros((8, 128), F32)
    for acc, (t, s) in zip(accs, pairs):
        val = jnp.sum(jnp.sum(acc, axis=0, keepdims=True), axis=1, keepdims=True)
        hit = ((row_id == t) & (col_id == s)) | ((row_id == s) & (col_id == t))
        gram = jnp.where(hit, val, gram)
    gram = all_reduce(7, gram)

    diag = jnp.where(row_id == col_id, gram, 0.0)
    scale = jnp.sum(jnp.sum(diag, axis=0, keepdims=True), axis=1, keepdims=True) / T
    w_row = jnp.where(col_id[0:1, :] < T, jnp.full((1, 128), 1.0 / T, F32), 0.0)
    w_col = jnp.where(row_id[:, 0:1] < T, jnp.full((8, 1), 1.0 / T, F32), 0.0)

    def solver(_, carry):
        wr, wc = carry
        pull_c = jnp.sum(gram * wr, axis=1, keepdims=True)
        pull_r = jnp.sum(gram * wc, axis=0, keepdims=True)
        rc = wc * jnp.exp(-pull_c / scale)
        rr = wr * jnp.exp(-pull_r / scale)
        return rr / jnp.sum(rr, axis=1, keepdims=True), rc / jnp.sum(rc, axis=0, keepdims=True)
    w_row, w_col = lax.fori_loop(0, SOLVER_STEPS, solver, (w_row, w_col))
    alpha_ref[...] = jnp.broadcast_to(w_row, (8, 128))

    alphas = [jnp.broadcast_to(w_col[t:t + 1, :], (8, 128)) for t in range(T)]

    def combine(k, _):
        tot = alphas[0] * shard[0, k]
        for t in range(1, T):
            tot = tot + alphas[t] * shard[t, k]
        gb[core, k] = tot
        return 0
    lax.fori_loop(0, nchunk, combine, 0)
    swap = pltpu.make_async_remote_copy(
        src_ref=gb.at[core], dst_ref=gb.at[core], send_sem=gs_sem, recv_sem=gr_sem,
        device_id=(partner,), device_id_type=MESH)
    swap.start()
    swap.wait()
    for h in range(2):
        for fb in range(nfb):
            tile = gb[h, 2 * fb + 1]
            rows = jnp.where(core == 0, tile[0:4], tile[4:8])
            for r in range(4):
                o = r * 2 * nfb + 2 * fb + h
                out1_ref[o:o + 1, :] = rows[r:r + 1]
        for rbl in range(rb_count // 2):
            for cb in range(2):
                tile = gb[h, 4 * ((rb_count // 2) * core + rbl) + 2 * cb]
                for r in range(8):
                    o = (8 * rbl + r) * 4 + 2 * cb + h
                    out2_ref[o:o + 1, :] = tile[r:r + 1]


def reduce_and_solve(cnt, aT, xT, dz, w2T, gp):
    rb, _, tok = aT.shape
    nchunk = 4 * rb
    any_spec = pl.BlockSpec(memory_space=pl.ANY)
    vm = pl.BlockSpec(memory_space=pltpu.VMEM)
    rows = 4 * rb * 512 // 128
    V = pltpu.VMEM
    DS = pltpu.SemaphoreType.DMA
    return pl.pallas_call(
        functools.partial(kernel, rb),
        name="grads_rs",
        out_shape=[jax.ShapeDtypeStruct((8, 128), F32), jax.ShapeDtypeStruct((rows, 128), F32), jax.ShapeDtypeStruct((rows, 128), F32)],
        in_specs=[vm] + [any_spec] * 5,
        out_specs=[vm] * 3,
        scratch_shapes=[
            V((rb, 512, tok), BF16), V((512, tok), BF16), V((T, tok, 512), BF16), V((2 * rb, 512, 256), BF16),
            V((2, tok, 256), F32), V((tok, 256), BF16), V((T, 8, 128), F32),
            V((2, 2, T, 512, 128), BF16), V((XRING, T, 512, 128), BF16),
            V((DEPTH, T, 4, 4, 4, 8, 128), F32), V((DEPTH, T, 4, 4, 8, 128), F32), V((DEPTH, T, 4, 8, 128), F32),
            V((RING, 3, T, 4, 4, 8, 128), F32), V((RING, 3, T, 4, 8, 128), F32), V((RING, 3, T, 8, 128), F32),
            V((T, nchunk, 8, 128), F32), V((2, nchunk, 8, 128), F32), V((14, 8, 128), F32), V((14, 8, 128), F32),
            DS((rb + T + 2,)), DS((2,)), DS((2, 2)), DS((XRING, 2)), DS((3, DEPTH)), DS((3, 2, RING)),
            DS((14,)), DS((14,)), DS, DS,
        ],
        compiler_params=pltpu.CompilerParams(collective_id=0, has_side_effects=True, vmem_limit_bytes=66 * 1000 * 1000),
    )(cnt, aT, xT, dz, w2T, gp)


def forward(x_loc, w_in, w_out, task_heads, lab_loc, mask_loc):
    pre_act = jnp.dot(x_loc, w_in, preferred_element_type=F32)
    act_out, gelu_slope = jax.jvp(jax.nn.gelu, (pre_act,), (jnp.ones_like(pre_act),))
    act_bf = act_out.astype(BF16)
    residual = x_loc.astype(F32) + jnp.dot(act_bf, w_out, preferred_element_type=F32)
    z_bf = residual.astype(BF16)
    logits = jnp.einsum("bd,tdc->tbc", z_bf, task_heads, preferred_element_type=F32)
    soft_prob = jax.nn.softmax(logits, axis=-1)
    onehot = (lab_loc[:, :, None] == jnp.arange(logits.shape[-1])).astype(F32)
    d_logit = (mask_loc[:, :, None].astype(F32) * (soft_prob - onehot)).astype(BF16)
    d_resid = jnp.einsum("tbc,tdc->tbd", d_logit, task_heads, preferred_element_type=F32).astype(BF16)
    return act_bf, gelu_slope, d_resid


def solution(mesh):
    def local_step(x_loc, w_in, w_out, task_heads, lab_loc, mask_loc):
        tok = x_loc.shape[0]
        hid = w_in.shape[1]
        rb = hid // 512
        cnt = mask_loc.sum(axis=1).astype(F32)
        cnt = jnp.broadcast_to(jnp.pad(cnt, (0, 2))[:, None], (8, 128))
        act, slope, dz = forward(x_loc, w_in, w_out, task_heads, lab_loc, mask_loc)
        aT = act.reshape(tok, 64, rb, 8).transpose(2, 1, 3, 0).reshape(rb, 512, tok)
        w2T = w_out.reshape(2 * rb, 256, 512).transpose(0, 2, 1)
        alpha, g_in, g_out = reduce_and_solve(cnt, aT, x_loc.T, dz, w2T, slope)
        return alpha[0, :6], g_in.reshape(-1), g_out.reshape(-1)

    return jax.shard_map(local_step, mesh=mesh, in_specs=(P("data", None), P(), P(), P(), P(None, "data"), P(None, "data")), out_specs=(P(), P("data"), P("data")), check_vma=False)
```

```python
import functools

import jax
import jax.numpy as jnp
from jax import lax
from jax.experimental import pallas as pl
from jax.experimental.pallas import tpu as pltpu
from jax.sharding import PartitionSpec as P

SOLVER_STEPS = 20
T = 6
MESH = pl.DeviceIdType.MESH
STRIDES = (32, 8, 2)
RING, DEPTH, XRING = 8, 4, 3
F32, BF16 = jnp.float32, jnp.bfloat16


def perm(order, z, y, x):
    return ((z, y, x), (y, x, z), (x, z, y))[order]


def kernel(rb_count, cnt_ref, aT_hbm, xT_hbm, dz_hbm, w2T_hbm, gp_hbm,
           alpha_ref, out1_ref, out2_ref,
           aT, xT, dz, w2T, gp, q, inv, hb, xr, dbuf, ebuf, fbuf, r1, r2, r3, shard, gb, ar_s, ar_r,
           ld_sem, gp_sem, xs_sem, xr_sem, s_sem, r_sem, ars_sem, arr_sem, gs_sem, gr_sem):
    nchunk = 4 * rb_count
    nfb = 2 * rb_count
    me = lax.axis_index("data")
    core = lax.rem(me, 2)
    coord = (lax.div(me, 32), lax.rem(lax.div(me, 8), 4), lax.rem(lax.div(me, 2), 4))
    partner = me + 1 - 2 * core

    def nb(dim, step):
        u = coord[dim]
        return (me + (lax.rem(u + step + 4, 4) - u) * STRIDES[dim],)

    def rel(dim, step):
        return lax.rem(coord[dim] + step + 4, 4)

    loads = [pltpu.make_async_copy(aT_hbm.at[i], aT.at[i], ld_sem.at[i]) for i in range(rb_count)]
    dz_loads = [pltpu.make_async_copy(dz_hbm.at[t], dz.at[t], ld_sem.at[rb_count + t]) for t in range(T)]
    x_load = pltpu.make_async_copy(xT_hbm, xT, ld_sem.at[rb_count + T])
    w_load = pltpu.make_async_copy(w2T_hbm, w2T, ld_sem.at[rb_count + T + 1])

    def gp_load(fb):
        cols = pl.ds(pl.multiple_of(fb * 256, 256), 256)
        return pltpu.make_async_copy(gp_hbm.at[:, cols], gp.at[lax.rem(fb, 2)], gp_sem.at[lax.rem(fb, 2)])

    loads[0].start()
    for c in dz_loads:
        c.start()
    w_load.start()
    x_load.start()
    gp_load(0).start()
    for c in loads[1:]:
        c.start()

    barrier = pltpu.get_barrier_semaphore()
    peers = [(partner,)] + [nb(d, s) for d in range(3) for s in (1, -1, 2)]
    for p in peers:
        pl.semaphore_signal(barrier, inc=1, device_id=p, device_id_type=MESH)
    pl.semaphore_wait(barrier, 10)

    def all_reduce(base, val):
        ar_s[base] = val
        cp = pltpu.make_async_remote_copy(
            src_ref=ar_s.at[base], dst_ref=ar_r.at[base, 0], send_sem=ars_sem.at[base], recv_sem=arr_sem.at[base],
            device_id=(partner,), device_id_type=MESH)
        cp.start()
        cp.wait()
        val = val + ar_r[base, 0]
        for dim in range(3):
            s = base + 1 + dim
            u = coord[dim]
            ar_s[s] = val
            for step in (2, 1, 3):
                pltpu.make_async_remote_copy(
                    src_ref=ar_s.at[s], dst_ref=ar_r.at[s, u], send_sem=ars_sem.at[s], recv_sem=arr_sem.at[s],
                    device_id=nb(dim, step), device_id_type=MESH).start()
            three = ar_r.at[s, pl.ds(0, 3)]
            pltpu.make_async_copy(three, three, arr_sem.at[s]).wait()
            pltpu.make_async_copy(three, three, ars_sem.at[s]).wait()
            part = [jnp.where(u == i, val, ar_r[s, i]) for i in range(4)]
            val = (part[0] + part[1]) + (part[2] + part[3])
        return val

    total = all_reduce(0, cnt_ref[...])
    inv_all = 1.0 / jnp.maximum(total, 1.0)
    for t in range(T):
        inv[t] = jnp.broadcast_to(inv_all[t:t + 1, :], (8, 128))

    srcs = (dbuf, ebuf, fbuf)
    recvs = (r1, r2, r3)

    def dims_of(p, t):
        return (t % 3 + p) % 3, (1 if t < 3 else -1)

    def drain_sends(p, d):
        ref = recvs[p].at[0]
        pltpu.make_async_copy(ref, ref, s_sem.at[p, d]).wait()

    def send(p, k, t, blk, kind, step, dim):
        slot, d = lax.rem(k, RING), lax.rem(k, DEPTH)
        pltpu.make_async_remote_copy(
            src_ref=srcs[p].at[d, t, blk], dst_ref=recvs[p].at[slot, kind, t],
            send_sem=s_sem.at[p, d], recv_sem=r_sem.at[p, 0 if kind == 0 else 1, slot],
            device_id=nb(dim, step), device_id_type=MESH).start()

    def open_phase(p, k):
        for t in range(T):
            dim, sg = dims_of(p, t)
            send(p, k, t, rel(dim, 2), 0, sg, dim)
        for t in range(T):
            dim, sg = dims_of(p, t)
            send(p, k, t, rel(dim, -sg), 1, -sg, dim)

    def relay(p, k):
        slot, d = lax.rem(k, RING), lax.rem(k, DEPTH)
        ref = recvs[p].at[slot, 0]
        pltpu.make_async_copy(ref, ref, r_sem.at[p, 0, slot]).wait()
        for t in range(T):
            dim, sg = dims_of(p, t)
            v = rel(dim, sg)
            srcs[p][d, t, v] = srcs[p][d, t, v] + recvs[p][slot, 0, t]
        for t in range(T):
            dim, sg = dims_of(p, t)
            send(p, k, t, rel(dim, sg), 2, sg, dim)

    def close(p, k):
        slot, d = lax.rem(k, RING), lax.rem(k, DEPTH)
        ref = recvs[p].at[slot, pl.ds(1, 2)]
        pltpu.make_async_copy(ref, ref, r_sem.at[p, 1, slot]).wait()
        if p < 2:
            @pl.when(k >= DEPTH)
            def _():
                drain_sends(p + 1, d)
        for t in range(T):
            dim, _ = dims_of(p, t)
            out = srcs[p][d, t, coord[dim]] + recvs[p][slot, 1, t] + recvs[p][slot, 2, t]
            if p < 2:
                srcs[p + 1][d, t] = out
            else:
                shard[t, k] = out
        if p < 2:
            open_phase(p + 1, k)

    def half_copy(k, half):
        hs, xs = lax.rem(k, 2), lax.rem(k, XRING)
        return pltpu.make_async_remote_copy(
            src_ref=hb.at[hs, 1 - core, pl.ds(3 * half, 3)], dst_ref=xr.at[xs, pl.ds(3 * half, 3)],
            send_sem=xs_sem.at[hs, half], recv_sem=xr_sem.at[xs, half],
            device_id=(partner,), device_id_type=MESH)

    def merge(k):
        d, hs, xs = lax.rem(k, DEPTH), lax.rem(k, 2), lax.rem(k, XRING)
        half_copy(k, 0).wait_recv()
        half_copy(k, 1).wait_recv()

        @pl.when(k >= DEPTH)
        def _():
            drain_sends(0, d)
        for t in range(T):
            for pair in range(32):
                rows = slice(16 * pair, 16 * pair + 16)
                s = hb[hs, core, t, rows, :].astype(F32) + xr[xs, t, rows, :].astype(F32)
                for e in range(2):
                    i = 2 * pair + e
                    a, b, c = perm(t % 3, i // 16, (i // 4) % 4, i % 4)
                    dbuf[d, t, a, b, c] = s[8 * e:8 * e + 8]
        open_phase(0, k)

    def emit(hs, t, acc):
        row = inv[t][0:1, :]
        hb[hs, 0, t] = (acc[:, :128] * row).astype(BF16)
        hb[hs, 1, t] = (acc[:, 128:] * row).astype(BF16)

    def compute_out(k, half):
        j = lax.div(k, 2)
        rb, cb = lax.div(j, 2), lax.rem(j, 2)
        hs = lax.rem(k, 2)
        cols = pl.ds(pl.multiple_of(cb * 256, 256), 256)
        if half == 0:
            for i in range(rb_count):
                @pl.when(j == 2 * i)
                def _():
                    loads[i].wait()

        @pl.when(k == 0)
        def _():
            for t in range(3):
                dz_loads[3 * half + t].wait()

        for t in range(3 * half, 3 * half + 3):
            acc = jnp.dot(aT[rb], dz[t, :, cols], preferred_element_type=F32)
            emit(hs, t, acc)

    def compute_in(k, half):
        fb = lax.div(k, 2)
        hs, gs = lax.rem(k, 2), lax.rem(fb, 2)
        if half == 0:
            @pl.when(k == 1)
            def _():
                w_load.wait()
                x_load.wait()
            gp_load(fb).wait()

            @pl.when(fb + 1 < nfb)
            def _():
                gp_load(fb + 1).start()

        for t in range(3 * half, 3 * half + 3):
            d_act = jnp.dot(dz[t], w2T[fb], preferred_element_type=F32)
            q[t % 2] = (d_act * gp[gs]).astype(BF16)
            acc = jnp.dot(xT[...], q[t % 2], preferred_element_type=F32)
            emit(hs, t, acc)

    def compute(k, half):
        @pl.when(k < nchunk)
        def _():
            if half == 0:
                @pl.when(k >= 2)
                def _():
                    half_copy(k, 0).wait_send()
                    half_copy(k, 1).wait_send()

            @pl.when(lax.rem(k, 2) == 0)
            def _():
                compute_out(k, half)

            @pl.when(lax.rem(k, 2) == 1)
            def _():
                compute_in(k, half)
            half_copy(k, half).start()

    def at(k, fn):
        @pl.when((k >= 0) & (k < nchunk))
        def _():
            fn(k)

    def slot(kk, _):
        at(kk - 3, functools.partial(relay, 0))
        at(kk - 6, functools.partial(relay, 1))
        at(kk - 9, functools.partial(relay, 2))
        compute(kk, 0)
        at(kk - 1, merge)
        at(kk - 4, functools.partial(close, 0))
        at(kk - 7, functools.partial(close, 1))
        at(kk - 10, functools.partial(close, 2))
        compute(kk, 1)
        return 0
    lax.fori_loop(0, nchunk + 10, slot, 0)

    for i in range(DEPTH):
        for p in range(3):
            drain_sends(p, i)
    for k in (nchunk - 2, nchunk - 1):
        half_copy(k, 0).wait_send()
        half_copy(k, 1).wait_send()

    pairs = [(t, s) for t in range(T) for s in range(t, T)]

    def gram_step(k, accs):
        rows = [shard[t, k] for t in range(T)]
        return tuple(acc + rows[t] * rows[s] for acc, (t, s) in zip(accs, pairs))
    accs = lax.fori_loop(0, nchunk, gram_step, tuple(jnp.zeros((8, 128), F32) for _ in pairs))
    row_id = lax.broadcasted_iota(jnp.int32, (8, 128), 0)
    col_id = lax.broadcasted_iota(jnp.int32, (8, 128), 1)
    gram = jnp.zeros((8, 128), F32)
    for acc, (t, s) in zip(accs, pairs):
        val = jnp.sum(jnp.sum(acc, axis=0, keepdims=True), axis=1, keepdims=True)
        hit = ((row_id == t) & (col_id == s)) | ((row_id == s) & (col_id == t))
        gram = jnp.where(hit, val, gram)
    gram = all_reduce(4, gram)

    diag = jnp.where(row_id == col_id, gram, 0.0)
    scale = jnp.sum(jnp.sum(diag, axis=0, keepdims=True), axis=1, keepdims=True) / T
    w_row = jnp.where(col_id[0:1, :] < T, jnp.full((1, 128), 1.0 / T, F32), 0.0)
    w_col = jnp.where(row_id[:, 0:1] < T, jnp.full((8, 1), 1.0 / T, F32), 0.0)

    def solver(_, carry):
        wr, wc = carry
        pull_c = jnp.sum(gram * wr, axis=1, keepdims=True)
        pull_r = jnp.sum(gram * wc, axis=0, keepdims=True)
        rc = wc * jnp.exp(-pull_c / scale)
        rr = wr * jnp.exp(-pull_r / scale)
        return rr / jnp.sum(rr, axis=1, keepdims=True), rc / jnp.sum(rc, axis=0, keepdims=True)
    w_row, w_col = lax.fori_loop(0, SOLVER_STEPS, solver, (w_row, w_col))
    alpha_ref[...] = jnp.broadcast_to(w_row, (8, 128))

    alphas = [jnp.broadcast_to(w_col[t:t + 1, :], (8, 128)) for t in range(T)]

    def combine(k, _):
        tot = alphas[0] * shard[0, k]
        for t in range(1, T):
            tot = tot + alphas[t] * shard[t, k]
        gb[core, k] = tot
        return 0
    lax.fori_loop(0, nchunk, combine, 0)
    swap = pltpu.make_async_remote_copy(
        src_ref=gb.at[core], dst_ref=gb.at[core], send_sem=gs_sem, recv_sem=gr_sem,
        device_id=(partner,), device_id_type=MESH)
    swap.start()
    swap.wait()
    for h in range(2):
        for fb in range(nfb):
            tile = gb[h, 2 * fb + 1]
            rows = jnp.where(core == 0, tile[0:4], tile[4:8])
            for r in range(4):
                o = r * 2 * nfb + 2 * fb + h
                out1_ref[o:o + 1, :] = rows[r:r + 1]
        for rbl in range(rb_count // 2):
            for cb in range(2):
                tile = gb[h, 4 * ((rb_count // 2) * core + rbl) + 2 * cb]
                for r in range(8):
                    o = (8 * rbl + r) * 4 + 2 * cb + h
                    out2_ref[o:o + 1, :] = tile[r:r + 1]


def reduce_and_solve(cnt, aT, xT, dz, w2T, gp):
    rb, _, tok = aT.shape
    nchunk = 4 * rb
    any_spec = pl.BlockSpec(memory_space=pl.ANY)
    vm = pl.BlockSpec(memory_space=pltpu.VMEM)
    rows = 4 * rb * 512 // 128
    V = pltpu.VMEM
    DS = pltpu.SemaphoreType.DMA
    return pl.pallas_call(
        functools.partial(kernel, rb),
        name="grads_rs",
        out_shape=[jax.ShapeDtypeStruct((8, 128), F32), jax.ShapeDtypeStruct((rows, 128), F32), jax.ShapeDtypeStruct((rows, 128), F32)],
        in_specs=[vm] + [any_spec] * 5,
        out_specs=[vm] * 3,
        scratch_shapes=[
            V((rb, 512, tok), BF16), V((512, tok), BF16), V((T, tok, 512), BF16), V((2 * rb, 512, 256), BF16),
            V((2, tok, 256), F32), V((2, tok, 256), BF16), V((T, 8, 128), F32),
            V((2, 2, T, 512, 128), BF16), V((XRING, T, 512, 128), BF16),
            V((DEPTH, T, 4, 4, 4, 8, 128), F32), V((DEPTH, T, 4, 4, 8, 128), F32), V((DEPTH, T, 4, 8, 128), F32),
            V((RING, 3, T, 4, 4, 8, 128), F32), V((RING, 3, T, 4, 8, 128), F32), V((RING, 3, T, 8, 128), F32),
            V((T, nchunk, 8, 128), F32), V((2, nchunk, 8, 128), F32), V((8, 8, 128), F32), V((8, 4, 8, 128), F32),
            DS((rb + T + 2,)), DS((2,)), DS((2, 2)), DS((XRING, 2)), DS((3, DEPTH)), DS((3, 2, RING)),
            DS((8,)), DS((8,)), DS, DS,
        ],
        compiler_params=pltpu.CompilerParams(collective_id=0, has_side_effects=True, vmem_limit_bytes=66 * 1000 * 1000),
    )(cnt, aT, xT, dz, w2T, gp)


def forward(x_loc, w_in, w_out, task_heads, lab_loc, mask_loc):
    pre_act = jnp.dot(x_loc, w_in, preferred_element_type=F32)
    act_out, gelu_slope = jax.jvp(jax.nn.gelu, (pre_act,), (jnp.ones_like(pre_act),))
    act_bf = act_out.astype(BF16)
    residual = x_loc.astype(F32) + jnp.dot(act_bf, w_out, preferred_element_type=F32)
    z_bf = residual.astype(BF16)
    logits = jnp.einsum("bd,tdc->tbc", z_bf, task_heads, preferred_element_type=F32)
    soft_prob = jax.nn.softmax(logits, axis=-1)
    onehot = (lab_loc[:, :, None] == jnp.arange(logits.shape[-1])).astype(F32)
    d_logit = (mask_loc[:, :, None].astype(F32) * (soft_prob - onehot)).astype(BF16)
    d_resid = jnp.einsum("tbc,tdc->tbd", d_logit, task_heads, preferred_element_type=F32).astype(BF16)
    return act_bf, gelu_slope, d_resid


def solution(mesh):
    def local_step(x_loc, w_in, w_out, task_heads, lab_loc, mask_loc):
        tok = x_loc.shape[0]
        hid = w_in.shape[1]
        rb = hid // 512
        cnt = mask_loc.sum(axis=1).astype(F32)
        cnt = jnp.broadcast_to(jnp.pad(cnt, (0, 2))[:, None], (8, 128))
        act, slope, dz = forward(x_loc, w_in, w_out, task_heads, lab_loc, mask_loc)
        aT = act.reshape(tok, 64, rb, 8).transpose(2, 1, 3, 0).reshape(rb, 512, tok)
        w2T = w_out.reshape(2 * rb, 256, 512).transpose(0, 2, 1)
        alpha, g_in, g_out = reduce_and_solve(cnt, aT, x_loc.T, dz, w2T, slope)
        return alpha[0, :6], g_in.reshape(-1), g_out.reshape(-1)

    return jax.shard_map(local_step, mesh=mesh, in_specs=(P("data", None), P(), P(), P(), P(None, "data"), P(None, "data")), out_specs=(P(), P("data"), P("data")), check_vma=False)
```

```python
import functools

import jax
import jax.numpy as jnp
from jax import lax
from jax.experimental import pallas as pl
from jax.experimental.pallas import tpu as pltpu
from jax.sharding import PartitionSpec as P

SOLVER_STEPS = 20
T = 6
MESH = pl.DeviceIdType.MESH
STRIDES = (32, 8, 2)
RING, DEPTH, XRING = 8, 4, 3
F32, BF16 = jnp.float32, jnp.bfloat16


def perm(order, z, y, x):
    return ((z, y, x), (y, x, z), (x, z, y))[order]


def kernel(code_ref, ht3_ref, ht24_ref, x_hbm, w1_hbm, w2_hbm,
           alpha_ref, out1_ref, out2_ref, gp_hbm,
           aT, xT, dz, w2, gp, q, hbig, inv, hb, xr, dbuf, ebuf, fbuf, r1, r2, r3, shard, gb, ar_s, ar_r,
           ld_sem, gp_sem, xs_sem, xr_sem, s_sem, r_sem, ars_sem, arr_sem, gs_sem, gr_sem):
    nchunk, nfb = 16, 8
    me = lax.axis_index("data")
    core = lax.rem(me, 2)
    coord = (lax.div(me, 32), lax.rem(lax.div(me, 8), 4), lax.rem(lax.div(me, 2), 4))
    partner = me + 1 - 2 * core

    def nb(dim, step):
        u = coord[dim]
        return (me + (lax.rem(u + step + 4, 4) - u) * STRIDES[dim],)

    def rel(dim, step):
        return lax.rem(coord[dim] + step + 4, 4)

    x_loads = [pltpu.make_async_copy(x_hbm.at[:, pl.ds(256 * i, 256)], q.at[i], ld_sem.at[i]) for i in range(2)]
    w1_load = pltpu.make_async_copy(w1_hbm, xT, ld_sem.at[2])
    w2_load = pltpu.make_async_copy(w2_hbm, w2, ld_sem.at[3])
    for c in x_loads + [w1_load, w2_load]:
        c.start()

    def gp_load(fb):
        return pltpu.make_async_copy(gp_hbm.at[fb], gp.at[lax.rem(fb, 2)], gp_sem.at[lax.rem(fb, 2)])

    def gp_store(fb):
        return pltpu.make_async_copy(gp.at[lax.rem(fb, 2)], gp_hbm.at[fb], gp_sem.at[lax.rem(fb, 2)])

    barrier = pltpu.get_barrier_semaphore()
    peers = [(partner,)] + [nb(d, s) for d in range(3) for s in (1, -1, 2)]
    for p in peers:
        pl.semaphore_signal(barrier, inc=1, device_id=p, device_id_type=MESH)
    pl.semaphore_wait(barrier, 10)

    def ar_core(base):
        return pltpu.make_async_remote_copy(
            src_ref=ar_s.at[base], dst_ref=ar_r.at[base, 0], send_sem=ars_sem.at[base], recv_sem=arr_sem.at[base],
            device_id=(partner,), device_id_type=MESH)

    def ar_start(base, stage, val):
        s = base + stage
        ar_s[s] = val
        if stage == 0:
            ar_core(base).start()
            return
        dim = stage - 1
        for step in (2, 1, 3):
            pltpu.make_async_remote_copy(
                src_ref=ar_s.at[s], dst_ref=ar_r.at[s, coord[dim]], send_sem=ars_sem.at[s], recv_sem=arr_sem.at[s],
                device_id=nb(dim, step), device_id_type=MESH).start()

    def ar_finish(base, stage):
        s = base + stage
        if stage == 0:
            ar_core(base).wait()
            return ar_s[s] + ar_r[s, 0]
        three = ar_r.at[s, pl.ds(0, 3)]
        pltpu.make_async_copy(three, three, arr_sem.at[s]).wait()
        pltpu.make_async_copy(three, three, ars_sem.at[s]).wait()
        u = coord[stage - 1]
        part = [jnp.where(u == i, ar_s[s], ar_r[s, i]) for i in range(4)]
        return (part[0] + part[1]) + (part[2] + part[3])

    def all_reduce(base, val):
        for stage in range(4):
            ar_start(base, stage, val)
            val = ar_finish(base, stage)
        return val

    cnt = jnp.sum((code_ref[0:8, :] >= 0).astype(F32), axis=1, keepdims=True)
    ar_start(0, 0, jnp.broadcast_to(cnt, (8, 128)))
    for c in x_loads + [w1_load]:
        c.wait()
    K0, K1 = 0.7978845608028654, 0.044715

    def hidden(fb, _):
        cols = pl.ds(pl.multiple_of(fb * 256, 256), 256)
        for stage in range(1, 4):
            @pl.when(fb == 2 * stage)
            def _():
                ar_start(0, stage, ar_finish(0, stage - 1))

        @pl.when(fb >= 2)
        def _():
            gp_store(fb - 2).wait()
        for i in range(4):
            rows = slice(512 * i, 512 * i + 512)
            p = (jnp.dot(q[0, rows, :], xT[0:256, cols], preferred_element_type=F32)
                 + jnp.dot(q[1, rows, :], xT[256:512, cols], preferred_element_type=F32))
            p2 = p * p
            th = jnp.tanh(p * (K0 + (K0 * K1) * p2))
            cdf = 0.5 + 0.5 * th
            act = (p * cdf).astype(BF16)
            gp[lax.rem(fb, 2), rows, :] = cdf + (0.5 - 0.5 * (th * th)) * (p * (K0 + (3 * K0 * K1) * p2))
            dz[lax.div(fb, 2), rows, pl.ds(pl.multiple_of(lax.rem(fb, 2) * 256, 256), 256)] = act
            aT[pl.ds(fb * 8, 8), :, :, rows] = act.T.reshape(8, 2, 16, 512)
        gp_store(fb).start()
        return 0
    lax.fori_loop(0, nfb, hidden, 0)
    gp_store(nfb - 2).wait()
    gp_store(nfb - 1).wait()
    gp_load(0).start()

    inv_all = 1.0 / jnp.maximum(ar_finish(0, 3), 1.0)
    for t in range(T):
        inv[t] = jnp.broadcast_to(inv_all[t:t + 1, :], (8, 128))

    head_row = lax.rem(lax.broadcasted_iota(jnp.int32, (128, 512), 0), 8)
    for t in range(T):
        hbig[t] = jnp.where(head_row == t, ht24_ref[...].astype(F32), 0.0).astype(BF16)
    w2_load.wait()

    def tokens(i, _):
        rows = pl.ds(pl.multiple_of(i * 512, 512), 512)
        z = jnp.dot(dz[0, rows, :], w2[0:512, :], preferred_element_type=F32)
        for j in range(1, 4):
            z = z + jnp.dot(dz[j, rows, :], w2[512 * j:512 * j + 512, :], preferred_element_type=F32)
        x_t = jnp.concatenate([q[0, rows, :], q[1, rows, :]], axis=1)
        zb = (x_t.astype(F32) + z).astype(BF16)
        logits = lax.dot_general(zb, ht3_ref[...], (((1,), (1,)), ((), ())), preferred_element_type=F32)
        ls = [logits[:, 128 * c:128 * c + 128] for c in range(3)]
        top = jnp.maximum(jnp.maximum(ls[0], ls[1]), ls[2])
        ex = [jnp.exp(v - top) for v in ls]
        den = ex[0] + ex[1] + ex[2]
        code = code_ref[:, rows].T
        errs = []
        for c in range(3):
            err = jnp.where(code >= 0, ex[c] / den - (code == c).astype(F32), 0.0)
            errs.append(err.astype(BF16).astype(F32))
        packed = (errs[0] + pltpu.roll(errs[1], 8, 1) + pltpu.roll(errs[2], 16, 1)).astype(BF16)
        for t in range(T):
            dz[t, rows, :] = jnp.dot(packed, hbig[t], preferred_element_type=F32).astype(BF16)
        xT[:, rows] = x_t.T
        return 0
    lax.fori_loop(0, 4, tokens, 0)

    srcs = (dbuf, ebuf, fbuf)
    recvs = (r1, r2, r3)

    def dims_of(p, t):
        return (t % 3 + p) % 3, (1 if t < 3 else -1)

    def drain_sends(p, d):
        ref = recvs[p].at[0]
        pltpu.make_async_copy(ref, ref, s_sem.at[p, d]).wait()

    def send(p, k, t, blk, kind, step, dim):
        slot, d = lax.rem(k, RING), lax.rem(k, DEPTH)
        pltpu.make_async_remote_copy(
            src_ref=srcs[p].at[d, t, blk], dst_ref=recvs[p].at[slot, kind, t],
            send_sem=s_sem.at[p, d], recv_sem=r_sem.at[p, 0 if kind == 0 else 1, slot],
            device_id=nb(dim, step), device_id_type=MESH).start()

    def open_phase(p, k):
        for t in range(T):
            dim, sg = dims_of(p, t)
            send(p, k, t, rel(dim, 2), 0, sg, dim)
        for t in range(T):
            dim, sg = dims_of(p, t)
            send(p, k, t, rel(dim, -sg), 1, -sg, dim)

    def relay(p, k):
        slot, d = lax.rem(k, RING), lax.rem(k, DEPTH)
        ref = recvs[p].at[slot, 0]
        pltpu.make_async_copy(ref, ref, r_sem.at[p, 0, slot]).wait()
        for t in range(T):
            dim, sg = dims_of(p, t)
            v = rel(dim, sg)
            srcs[p][d, t, v] = srcs[p][d, t, v] + recvs[p][slot, 0, t]
        for t in range(T):
            dim, sg = dims_of(p, t)
            send(p, k, t, rel(dim, sg), 2, sg, dim)

    def close(p, k):
        slot, d = lax.rem(k, RING), lax.rem(k, DEPTH)
        ref = recvs[p].at[slot, pl.ds(1, 2)]
        pltpu.make_async_copy(ref, ref, r_sem.at[p, 1, slot]).wait()
        if p < 2:
            @pl.when(k >= DEPTH)
            def _():
                drain_sends(p + 1, d)
        for t in range(T):
            dim, _ = dims_of(p, t)
            out = srcs[p][d, t, coord[dim]] + recvs[p][slot, 1, t] + recvs[p][slot, 2, t]
            if p < 2:
                srcs[p + 1][d, t] = out
            else:
                shard[t, k] = out
        if p < 2:
            open_phase(p + 1, k)

    def half_copy(k, half):
        hs, xs = lax.rem(k, 2), lax.rem(k, XRING)
        return pltpu.make_async_remote_copy(
            src_ref=hb.at[hs, 1 - core, pl.ds(4 * half, 4 - 2 * half)], dst_ref=xr.at[xs, pl.ds(4 * half, 4 - 2 * half)],
            send_sem=xs_sem.at[hs, half], recv_sem=xr_sem.at[xs, half],
            device_id=(partner,), device_id_type=MESH)

    def merge(k):
        d, hs, xs = lax.rem(k, DEPTH), lax.rem(k, 2), lax.rem(k, XRING)
        half_copy(k, 0).wait_recv()
        half_copy(k, 1).wait_recv()

        @pl.when(k >= DEPTH)
        def _():
            drain_sends(0, d)
        for t in range(T):
            for pair in range(32):
                rows = slice(16 * pair, 16 * pair + 16)
                s = hb[hs, core, t, rows, :].astype(F32) + xr[xs, t, rows, :].astype(F32)
                for e in range(2):
                    i = 2 * pair + e
                    a, b, c = perm(t % 3, i // 16, (i // 4) % 4, i % 4)
                    dbuf[d, t, a, b, c] = s[8 * e:8 * e + 8]
        open_phase(0, k)

    def compute_out(k, half):
        j = lax.div(k, 2)
        h, cb = lax.div(j, 4), lax.rem(j, 4)
        hs = lax.rem(k, 2)
        cols = pl.ds(pl.multiple_of(cb * 128, 128), 128)
        lhs = aT[:, h, :, :].reshape(1024, 2048)
        for t in ((0, 2), (4,))[half]:
            rhs = jnp.concatenate([dz[t, :, cols], dz[t + 1, :, cols]], axis=1)
            acc = jnp.dot(lhs, rhs, preferred_element_type=F32)
            for e in range(2):
                part = (acc[:, 128 * e:128 * e + 128] * inv[t + e][0:1, :]).reshape(64, 2, 8, 128)
                for c in range(2):
                    hb[hs, c, t + e] = part[:, c].reshape(512, 128).astype(BF16)

    def compute_in(k, half):
        fb = lax.div(k, 2)
        hs, gs = lax.rem(k, 2), lax.rem(fb, 2)
        if half == 0:
            gp_load(fb).wait()

            @pl.when(fb + 1 < nfb)
            def _():
                gp_load(fb + 1).start()
        w_blk = w2[pl.ds(pl.multiple_of(fb * 256, 256), 256), :]
        for t in range(4 * half, 4 + 2 * half):
            d_act = lax.dot_general(dz[t], w_blk, (((1,), (1,)), ((), ())), preferred_element_type=F32)
            q[t % 2] = (d_act * gp[gs]).astype(BF16)
            acc = jnp.dot(xT[...], q[t % 2], preferred_element_type=F32)
            row = inv[t][0:1, :]
            hb[hs, 0, t] = (acc[:, :128] * row).astype(BF16)
            hb[hs, 1, t] = (acc[:, 128:] * row).astype(BF16)

    def compute(k, half):
        @pl.when(k < nchunk)
        def _():
            if half == 0:
                @pl.when(k >= 2)
                def _():
                    half_copy(k, 0).wait_send()
                    half_copy(k, 1).wait_send()

            @pl.when(lax.rem(k, 2) == 0)
            def _():
                compute_out(k, half)

            @pl.when(lax.rem(k, 2) == 1)
            def _():
                compute_in(k, half)
            half_copy(k, half).start()

    def at(k, fn):
        @pl.when((k >= 0) & (k < nchunk))
        def _():
            fn(k)

    def slot(kk, _):
        at(kk - 3, functools.partial(relay, 0))
        at(kk - 6, functools.partial(relay, 1))
        at(kk - 9, functools.partial(relay, 2))
        compute(kk, 0)
        at(kk - 1, merge)
        at(kk - 4, functools.partial(close, 0))
        at(kk - 7, functools.partial(close, 1))
        at(kk - 10, functools.partial(close, 2))
        compute(kk, 1)
        return 0
    lax.fori_loop(0, nchunk + 10, slot, 0)

    for i in range(DEPTH):
        for p in range(3):
            drain_sends(p, i)
    for k in (nchunk - 2, nchunk - 1):
        half_copy(k, 0).wait_send()
        half_copy(k, 1).wait_send()

    pairs = [(t, s) for t in range(T) for s in range(t, T)]

    def gram_step(k, accs):
        rows = [shard[t, k] for t in range(T)]
        return tuple(acc + rows[t] * rows[s] for acc, (t, s) in zip(accs, pairs))
    accs = lax.fori_loop(0, nchunk, gram_step, tuple(jnp.zeros((8, 128), F32) for _ in pairs))
    row_id = lax.broadcasted_iota(jnp.int32, (8, 128), 0)
    col_id = lax.broadcasted_iota(jnp.int32, (8, 128), 1)
    gram = jnp.zeros((8, 128), F32)
    for acc, (t, s) in zip(accs, pairs):
        val = jnp.sum(jnp.sum(acc, axis=0, keepdims=True), axis=1, keepdims=True)
        hit = ((row_id == t) & (col_id == s)) | ((row_id == s) & (col_id == t))
        gram = jnp.where(hit, val, gram)
    gram = all_reduce(4, gram)

    diag = jnp.where(row_id == col_id, gram, 0.0)
    scale = jnp.sum(jnp.sum(diag, axis=0, keepdims=True), axis=1, keepdims=True) / T
    w_row = jnp.where(col_id[0:1, :] < T, jnp.full((1, 128), 1.0 / T, F32), 0.0)
    w_col = jnp.where(row_id[:, 0:1] < T, jnp.full((8, 1), 1.0 / T, F32), 0.0)

    def solver(_, carry):
        wr, wc = carry
        pull_c = jnp.sum(gram * wr, axis=1, keepdims=True)
        pull_r = jnp.sum(gram * wc, axis=0, keepdims=True)
        rc = wc * jnp.exp(-pull_c / scale)
        rr = wr * jnp.exp(-pull_r / scale)
        return rr / jnp.sum(rr, axis=1, keepdims=True), rc / jnp.sum(rc, axis=0, keepdims=True)
    w_row, w_col = lax.fori_loop(0, SOLVER_STEPS, solver, (w_row, w_col))
    alpha_ref[...] = jnp.broadcast_to(w_row, (8, 128))

    alphas = [jnp.broadcast_to(w_col[t:t + 1, :], (8, 128)) for t in range(T)]

    def combine(k, _):
        tot = alphas[0] * shard[0, k]
        for t in range(1, T):
            tot = tot + alphas[t] * shard[t, k]
        gb[core, k] = tot
        return 0
    lax.fori_loop(0, nchunk, combine, 0)
    swap = pltpu.make_async_remote_copy(
        src_ref=gb.at[core], dst_ref=gb.at[core], send_sem=gs_sem, recv_sem=gr_sem,
        device_id=(partner,), device_id_type=MESH)
    swap.start()
    swap.wait()
    for h in range(2):
        for fb in range(nfb):
            tile = gb[h, 2 * fb + 1]
            rows = jnp.where(core == 0, tile[0:4], tile[4:8])
            for r in range(4):
                o = r * 2 * nfb + 2 * fb + h
                out1_ref[o:o + 1, :] = rows[r:r + 1]
        for cb in range(4):
            tile = gb[h, 2 * (4 * core + cb)]
            for r in range(8):
                o = (8 * h + r) * 4 + cb
                out2_ref[o:o + 1, :] = tile[r:r + 1]


def reduce_and_solve(code, ht3, ht24, x_loc, w_in, w_out):
    any_spec = pl.BlockSpec(memory_space=pl.ANY)
    vm = pl.BlockSpec(memory_space=pltpu.VMEM)
    V = pltpu.VMEM
    DS = pltpu.SemaphoreType.DMA
    shapes = [(8, 128), (64, 128), (64, 128), (8, 2048, 256)]
    return pl.pallas_call(
        kernel,
        name="grads_rs",
        out_shape=[jax.ShapeDtypeStruct(s, F32) for s in shapes],
        in_specs=[vm] * 3 + [any_spec] * 3,
        out_specs=[vm] * 3 + [any_spec],
        scratch_shapes=[
            V((64, 2, 16, 2048), BF16), V((512, 2048), BF16), V((T, 2048, 512), BF16), V((2048, 512), BF16),
            V((2, 2048, 256), F32), V((2, 2048, 256), BF16), V((T, 128, 512), BF16), V((T, 8, 128), F32),
            V((2, 2, T, 512, 128), BF16), V((XRING, T, 512, 128), BF16),
            V((DEPTH, T, 4, 4, 4, 8, 128), F32), V((DEPTH, T, 4, 4, 8, 128), F32), V((DEPTH, T, 4, 8, 128), F32),
            V((RING, 3, T, 4, 4, 8, 128), F32), V((RING, 3, T, 4, 8, 128), F32), V((RING, 3, T, 8, 128), F32),
            V((T, 16, 8, 128), F32), V((2, 16, 8, 128), F32), V((8, 8, 128), F32), V((8, 4, 8, 128), F32),
            DS((4,)), DS((2,)), DS((2, 2)), DS((XRING, 2)), DS((3, DEPTH)), DS((3, 2, RING)),
            DS((8,)), DS((8,)), DS, DS,
        ],
        compiler_params=pltpu.CompilerParams(collective_id=0, has_side_effects=True, vmem_limit_bytes=67043328),
    )(code, ht3, ht24, x_loc, w_in, w_out)


def solution(mesh):
    def local_step(x_loc, w_in, w_out, task_heads, lab_loc, mask_loc):
        code = jnp.where(mask_loc > 0, lab_loc, -1).astype(F32)
        code = jnp.pad(code, ((0, 122), (0, 0)), constant_values=-1.0)
        by_class = task_heads.transpose(2, 0, 1)
        ht3 = jnp.pad(by_class, ((0, 0), (0, 122), (0, 0))).reshape(384, 512)
        ht24 = jnp.pad(by_class, ((0, 0), (0, 2), (0, 0))).reshape(24, 512)
        ht24 = jnp.pad(ht24, ((0, 104), (0, 0)))
        alpha, g_in, g_out, _ = reduce_and_solve(code, ht3, ht24, x_loc, w_in, w_out)
        return alpha[0, :6], g_in.reshape(-1), g_out.reshape(-1)

    return jax.shard_map(local_step, mesh=mesh, in_specs=(P("data", None), P(), P(), P(), P(None, "data"), P(None, "data")), out_specs=(P(), P("data"), P("data")), check_vma=False)
```

```python
import functools

import jax
import jax.numpy as jnp
from jax import lax
from jax.experimental import pallas as pl
from jax.experimental.pallas import tpu as pltpu
from jax.sharding import PartitionSpec as P

SOLVER_STEPS = 20
T = 6
MESH = pl.DeviceIdType.MESH
STRIDES = (32, 8, 2)
RING, DEPTH, XRING = 8, 4, 3
F32, BF16 = jnp.float32, jnp.bfloat16


def perm(order, z, y, x):
    return ((z, y, x), (y, x, z), (x, z, y))[order]


def kernel(lab_ref, mask_ref, ht24_ref, x_hbm, w1_hbm, w2_hbm,
           alpha_ref, out1_ref, out2_ref, gp_hbm,
           aT, xT, dz, w2, gp, q, hbig, code_ref, ht3_ref, other, inv, hb, xr, dbuf, ebuf, fbuf, r1, r2, r3, shard, gb, ar_s, ar_r,
           ld_sem, gp_sem, xs_sem, xr_sem, s_sem, r_sem, ars_sem, arr_sem, gs_sem, gr_sem):
    nchunk, nfb = 16, 8
    me = lax.axis_index("data")
    core = lax.rem(me, 2)
    coord = (lax.div(me, 32), lax.rem(lax.div(me, 8), 4), lax.rem(lax.div(me, 2), 4))
    partner = me + 1 - 2 * core

    def nb(dim, step):
        u = coord[dim]
        return (me + (lax.rem(u + step + 4, 4) - u) * STRIDES[dim],)

    def rel(dim, step):
        return lax.rem(coord[dim] + step + 4, 4)

    x_loads = [pltpu.make_async_copy(x_hbm.at[:, pl.ds(256 * i, 256)], q.at[i], ld_sem.at[i]) for i in range(2)]
    w1_load = pltpu.make_async_copy(w1_hbm, xT, ld_sem.at[2])
    w2_load = pltpu.make_async_copy(w2_hbm, w2, ld_sem.at[3])
    for c in x_loads + [w1_load, w2_load]:
        c.start()

    def gp_load(fb):
        return pltpu.make_async_copy(gp_hbm.at[fb], gp.at[lax.rem(fb, 2)], gp_sem.at[lax.rem(fb, 2)])

    def gp_store(fb):
        return pltpu.make_async_copy(gp.at[lax.rem(fb, 2)], gp_hbm.at[fb], gp_sem.at[lax.rem(fb, 2)])

    barrier = pltpu.get_barrier_semaphore()
    peers = [(partner,)] + [nb(d, s) for d in range(3) for s in (1, -1, 2)]
    for p in peers:
        pl.semaphore_signal(barrier, inc=1, device_id=p, device_id_type=MESH)
    pl.semaphore_wait(barrier, 10)

    def ar_core(base):
        return pltpu.make_async_remote_copy(
            src_ref=ar_s.at[base], dst_ref=ar_r.at[base, 0], send_sem=ars_sem.at[base], recv_sem=arr_sem.at[base],
            device_id=(partner,), device_id_type=MESH)

    def ar_start(base, stage, val):
        s = base + stage
        ar_s[s] = val
        if stage == 0:
            ar_core(base).start()
            return
        dim = stage - 1
        for step in (2, 1, 3):
            pltpu.make_async_remote_copy(
                src_ref=ar_s.at[s], dst_ref=ar_r.at[s, coord[dim]], send_sem=ars_sem.at[s], recv_sem=arr_sem.at[s],
                device_id=nb(dim, step), device_id_type=MESH).start()

    def ar_finish(base, stage):
        s = base + stage
        if stage == 0:
            ar_core(base).wait()
            return ar_s[s] + ar_r[s, 0]
        three = ar_r.at[s, pl.ds(0, 3)]
        pltpu.make_async_copy(three, three, arr_sem.at[s]).wait()
        pltpu.make_async_copy(three, three, ars_sem.at[s]).wait()
        u = coord[stage - 1]
        part = [jnp.where(u == i, ar_s[s], ar_r[s, i]) for i in range(4)]
        return (part[0] + part[1]) + (part[2] + part[3])

    def all_reduce(base, val):
        for stage in range(4):
            ar_start(base, stage, val)
            val = ar_finish(base, stage)
        return val

    code_ref[...] = jnp.full(code_ref.shape, -1.0, F32)
    code_ref[0:T, :] = jnp.where(mask_ref[...] > 0, lab_ref[...], -1).astype(F32)
    cnt = jnp.sum((code_ref[0:8, :] >= 0).astype(F32), axis=1, keepdims=True)
    ar_start(0, 0, jnp.broadcast_to(cnt, (8, 128)))
    for c in x_loads + [w1_load]:
        c.wait()
    K0, K1 = 0.7978845608028654, 0.044715

    def hidden(fb, _):
        cols = pl.ds(pl.multiple_of(fb * 256, 256), 256)
        for stage in range(1, 4):
            @pl.when(fb == 2 * stage)
            def _():
                ar_start(0, stage, ar_finish(0, stage - 1))

        @pl.when(fb >= 2)
        def _():
            gp_store(fb - 2).wait()
        for i in range(4):
            rows = slice(512 * i, 512 * i + 512)
            p = (jnp.dot(q[0, rows, :], xT[0:256, cols], preferred_element_type=F32)
                 + jnp.dot(q[1, rows, :], xT[256:512, cols], preferred_element_type=F32))
            p2 = p * p
            th = jnp.tanh(p * (K0 + (K0 * K1) * p2))
            cdf = 0.5 + 0.5 * th
            act = (p * cdf).astype(BF16)
            gp[lax.rem(fb, 2), rows, :] = cdf + (0.5 - 0.5 * (th * th)) * (p * (K0 + (3 * K0 * K1) * p2))
            dz[lax.div(fb, 2), rows, pl.ds(pl.multiple_of(lax.rem(fb, 2) * 256, 256), 256)] = act
            aT[pl.ds(fb * 8, 8), :, :, rows] = act.T.reshape(8, 2, 16, 512)

        @pl.when(fb < nfb - 2)
        def _():
            gp_store(fb).start()
        return 0
    lax.fori_loop(0, nfb, hidden, 0)

    inv_all = 1.0 / jnp.maximum(ar_finish(0, 3), 1.0)
    for t in range(T):
        inv[t] = jnp.broadcast_to(inv_all[t:t + 1, :], (8, 128))

    heads = ht24_ref[...].astype(F32)
    for c in range(3):
        ht3_ref[128 * c:128 * c + 128, :] = jnp.concatenate([heads[8 * c:8 * c + 8], jnp.zeros((120, 512), F32)], axis=0).astype(BF16)
    head_row = lax.rem(lax.broadcasted_iota(jnp.int32, (128, 512), 0), 8)
    for t in range(T):
        hbig[t] = jnp.where(head_row == t, heads, 0.0).astype(BF16)
    w2_load.wait()

    def tokens(i, _):
        rows = pl.ds(pl.multiple_of(i * 512, 512), 512)
        z = jnp.dot(dz[0, rows, :], w2[0:512, :], preferred_element_type=F32)
        for j in range(1, 4):
            z = z + jnp.dot(dz[j, rows, :], w2[512 * j:512 * j + 512, :], preferred_element_type=F32)
        x_t = jnp.concatenate([q[0, rows, :], q[1, rows, :]], axis=1)
        zb = (x_t.astype(F32) + z).astype(BF16)
        logits = lax.dot_general(zb, ht3_ref[...], (((1,), (1,)), ((), ())), preferred_element_type=F32)
        ls = [logits[:, 128 * c:128 * c + 128] for c in range(3)]
        top = jnp.maximum(jnp.maximum(ls[0], ls[1]), ls[2])
        ex = [jnp.exp(v - top) for v in ls]
        den = ex[0] + ex[1] + ex[2]
        code = code_ref[:, rows].T
        errs = []
        for c in range(3):
            err = jnp.where(code >= 0, ex[c] / den - (code == c).astype(F32), 0.0)
            errs.append(err.astype(BF16).astype(F32))
        packed = (errs[0] + pltpu.roll(errs[1], 8, 1) + pltpu.roll(errs[2], 16, 1)).astype(BF16)
        for t in range(T):
            dz[t, rows, :] = jnp.dot(packed, hbig[t], preferred_element_type=F32).astype(BF16)
        xT[:, rows] = x_t.T
        return 0
    lax.fori_loop(0, 4, tokens, 0)

    srcs = (dbuf, ebuf, fbuf)
    recvs = (r1, r2, r3)

    def dims_of(p, t):
        return (t % 3 + p) % 3, (1 if t < 3 else -1)

    def drain_sends(p, d):
        ref = recvs[p].at[0]
        pltpu.make_async_copy(ref, ref, s_sem.at[p, d]).wait()

    def send(p, k, t, blk, kind, step, dim):
        slot, d = lax.rem(k, RING), lax.rem(k, DEPTH)
        pltpu.make_async_remote_copy(
            src_ref=srcs[p].at[d, t, blk], dst_ref=recvs[p].at[slot, kind, t],
            send_sem=s_sem.at[p, d], recv_sem=r_sem.at[p, 0 if kind == 0 else 1, slot],
            device_id=nb(dim, step), device_id_type=MESH).start()

    def open_phase(p, k):
        for t in range(T):
            dim, sg = dims_of(p, t)
            send(p, k, t, rel(dim, 2), 0, sg, dim)
        for t in range(T):
            dim, sg = dims_of(p, t)
            send(p, k, t, rel(dim, -sg), 1, -sg, dim)

    def relay(p, k):
        slot, d = lax.rem(k, RING), lax.rem(k, DEPTH)
        ref = recvs[p].at[slot, 0]
        pltpu.make_async_copy(ref, ref, r_sem.at[p, 0, slot]).wait()
        for t in range(T):
            dim, sg = dims_of(p, t)
            v = rel(dim, sg)
            srcs[p][d, t, v] = srcs[p][d, t, v] + recvs[p][slot, 0, t]
        for t in range(T):
            dim, sg = dims_of(p, t)
            send(p, k, t, rel(dim, sg), 2, sg, dim)

    def close(p, k):
        slot, d = lax.rem(k, RING), lax.rem(k, DEPTH)
        ref = recvs[p].at[slot, pl.ds(1, 2)]
        pltpu.make_async_copy(ref, ref, r_sem.at[p, 1, slot]).wait()
        if p < 2:
            @pl.when(k >= DEPTH)
            def _():
                drain_sends(p + 1, d)
        for t in range(T):
            dim, _ = dims_of(p, t)
            out = srcs[p][d, t, coord[dim]] + recvs[p][slot, 1, t] + recvs[p][slot, 2, t]
            if p < 2:
                srcs[p + 1][d, t] = out
            else:
                shard[t, k] = out
        if p < 2:
            open_phase(p + 1, k)

    def pair_copy(k, third):
        hs, xs = lax.rem(k, 2), lax.rem(k, XRING)
        return pltpu.make_async_remote_copy(
            src_ref=hb.at[hs, 1 - core, pl.ds(2 * third, 2)], dst_ref=xr.at[xs, pl.ds(2 * third, 2)],
            send_sem=xs_sem.at[hs, third], recv_sem=xr_sem.at[xs, third],
            device_id=(partner,), device_id_type=MESH)

    def merge(k):
        d, hs, xs = lax.rem(k, DEPTH), lax.rem(k, 2), lax.rem(k, XRING)
        for third in range(3):
            pair_copy(k, third).wait_recv()

        @pl.when(k >= DEPTH)
        def _():
            drain_sends(0, d)
        for t in range(T):
            for pair in range(32):
                rows = slice(16 * pair, 16 * pair + 16)
                s = hb[hs, core, t, rows, :].astype(F32) + xr[xs, t, rows, :].astype(F32)
                for e in range(2):
                    i = 2 * pair + e
                    a, b, c = perm(t % 3, i // 16, (i // 4) % 4, i % 4)
                    dbuf[d, t, a, b, c] = s[8 * e:8 * e + 8]
        open_phase(0, k)

    def compute_out(k, third):
        j = lax.div(k, 2)
        h, cb = lax.div(j, 4), lax.rem(j, 4)
        hs, t = lax.rem(k, 2), 2 * third
        cols = pl.ds(pl.multiple_of(cb * 128, 128), 128)
        lhs = aT[:, h, :, :].reshape(1024, 2048)
        rhs = jnp.concatenate([dz[t, :, cols], dz[t + 1, :, cols]], axis=1)
        acc = jnp.dot(lhs, rhs, preferred_element_type=F32)
        for e in range(2):
            part = (acc[:, 128 * e:128 * e + 128] * inv[t + e][0:1, :]).reshape(64, 2, 8, 128)
            for c in range(2):
                hb[hs, c, t + e] = part[:, c].reshape(512, 128).astype(BF16)

    def compute_in(k, third):
        fb = lax.rem(lax.div(k, 2) + nfb - 2, nfb)
        hs, gs, t = lax.rem(k, 2), lax.rem(fb, 2), 2 * third

        @pl.when((third == 0) & (fb < nfb - 2))
        def _():
            gp_load(fb).wait()

        @pl.when((third == 0) & (fb != nfb - 2) & (fb != nfb - 3))
        def _():
            gp_load(lax.rem(fb + 1, nfb)).start()
        w_blk = w2[pl.ds(pl.multiple_of(fb * 256, 256), 256), :]
        for e in range(2):
            d_act = lax.dot_general(dz[t + e], w_blk, (((1,), (1,)), ((), ())), preferred_element_type=F32)
            q[e] = (d_act * gp[gs]).astype(BF16)
        for e in range(2):
            acc = jnp.dot(xT[...], q[e], preferred_element_type=F32)
            row = inv[t + e][0:1, :]
            hb[hs, 0, t + e] = (acc[:, :128] * row).astype(BF16)
            hb[hs, 1, t + e] = (acc[:, 128:] * row).astype(BF16)

    def compute(k, third):
        @pl.when(k < nchunk)
        def _():
            @pl.when((third == 0) & (k >= 2))
            def _():
                for i in range(3):
                    pair_copy(k, i).wait_send()

            @pl.when(lax.rem(k, 2) == 0)
            def _():
                compute_out(k, third)

            @pl.when(lax.rem(k, 2) == 1)
            def _():
                compute_in(k, third)
            pair_copy(k, third).start()

    def at(third, want, k, fn):
        @pl.when((third == want) & (k >= 0) & (k < nchunk))
        def _():
            fn(k)

    def step(u, _):
        kk, third = lax.div(u, 3), lax.rem(u, 3)
        at(third, 0, kk - 3, functools.partial(relay, 0))
        at(third, 0, kk - 6, functools.partial(relay, 1))
        at(third, 0, kk - 9, functools.partial(relay, 2))
        at(third, 1, kk - 1, merge)
        at(third, 1, kk - 4, functools.partial(close, 0))
        at(third, 1, kk - 7, functools.partial(close, 1))
        at(third, 1, kk - 10, functools.partial(close, 2))
        compute(kk, third)
        return 0
    lax.fori_loop(0, 3 * (nchunk + 10), step, 0)

    for i in range(DEPTH):
        for p in range(3):
            drain_sends(p, i)
    for k in (nchunk - 2, nchunk - 1):
        for third in range(3):
            pair_copy(k, third).wait_send()

    swap = pltpu.make_async_remote_copy(
        src_ref=shard, dst_ref=other, send_sem=gs_sem, recv_sem=gr_sem,
        device_id=(partner,), device_id_type=MESH)
    swap.start()

    pairs = [(t, s) for t in range(T) for s in range(t, T)]

    def gram_step(k, accs):
        rows = [shard[t, k] for t in range(T)]
        return tuple(acc + rows[t] * rows[s] for acc, (t, s) in zip(accs, pairs))
    accs = lax.fori_loop(0, nchunk, gram_step, tuple(jnp.zeros((8, 128), F32) for _ in pairs))
    row_id = lax.broadcasted_iota(jnp.int32, (8, 128), 0)
    col_id = lax.broadcasted_iota(jnp.int32, (8, 128), 1)
    gram = jnp.zeros((8, 128), F32)
    for acc, (t, s) in zip(accs, pairs):
        val = jnp.sum(jnp.sum(acc, axis=0, keepdims=True), axis=1, keepdims=True)
        hit = ((row_id == t) & (col_id == s)) | ((row_id == s) & (col_id == t))
        gram = jnp.where(hit, val, gram)
    gram = all_reduce(4, gram)

    def entry(t, s):
        return jnp.broadcast_to(gram[t:t + 1, s:s + 1], (8, 128))
    upper = {(t, s): entry(t, s) for t, s in pairs}
    scale = upper[0, 0]
    for t in range(1, T):
        scale = scale + upper[t, t]
    scale = scale / T

    def tree(v):
        return (v[0] + v[1]) + (v[2] + v[3]) + (v[4] + v[5])

    def solver(_, w):
        raised = []
        for t in range(T):
            pull = tree([upper[min(t, s), max(t, s)] * w[s] for s in range(T)])
            raised.append(w[t] * jnp.exp(-pull / scale))
        tot = tree(raised)
        return tuple(r / tot for r in raised)
    alphas = lax.fori_loop(0, SOLVER_STEPS, solver, tuple(jnp.full((8, 128), 1.0 / T, F32) for _ in range(T)))
    packed = jnp.zeros((8, 128), F32)
    for t in range(T):
        packed = jnp.where(col_id == t, alphas[t], packed)
    alpha_ref[...] = packed
    swap.wait()

    def combine(k, _):
        for ref, who in ((shard, core), (other, 1 - core)):
            gb[who, k] = tree([alphas[t] * ref[t, k] for t in range(T)])
        return 0
    lax.fori_loop(0, nchunk, combine, 0)
    for h in range(2):
        for fb in range(nfb):
            tile = gb[h, 2 * ((fb + 2) % nfb) + 1]
            rows = jnp.where(core == 0, tile[0:4], tile[4:8])
            for r in range(4):
                o = r * 2 * nfb + 2 * fb + h
                out1_ref[o:o + 1, :] = rows[r:r + 1]
        for cb in range(4):
            tile = gb[h, 2 * (4 * core + cb)]
            for r in range(8):
                o = (8 * h + r) * 4 + cb
                out2_ref[o:o + 1, :] = tile[r:r + 1]


def reduce_and_solve(lab, mask, ht24, x_loc, w_in, w_out):
    any_spec = pl.BlockSpec(memory_space=pl.ANY)
    vm = pl.BlockSpec(memory_space=pltpu.VMEM)
    V = pltpu.VMEM
    DS = pltpu.SemaphoreType.DMA
    shapes = [(8, 128), (64, 128), (64, 128), (8, 2048, 256)]
    return pl.pallas_call(
        kernel,
        name="grads_rs",
        out_shape=[jax.ShapeDtypeStruct(s, F32) for s in shapes],
        in_specs=[vm] * 3 + [any_spec] * 3,
        out_specs=[vm] * 3 + [any_spec],
        scratch_shapes=[
            V((64, 2, 16, 2048), BF16), V((512, 2048), BF16), V((T, 2048, 512), BF16), V((2048, 512), BF16),
            V((2, 2048, 256), F32), V((2, 2048, 256), BF16), V((T, 128, 512), BF16),
            V((128, 2048), F32), V((384, 512), BF16), V((T, 16, 8, 128), F32), V((T, 8, 128), F32),
            V((2, 2, T, 512, 128), BF16), V((XRING, T, 512, 128), BF16),
            V((DEPTH, T, 4, 4, 4, 8, 128), F32), V((DEPTH, T, 4, 4, 8, 128), F32), V((DEPTH, T, 4, 8, 128), F32),
            V((RING, 3, T, 4, 4, 8, 128), F32), V((RING, 3, T, 4, 8, 128), F32), V((RING, 3, T, 8, 128), F32),
            V((T, 16, 8, 128), F32), V((2, 16, 8, 128), F32), V((8, 8, 128), F32), V((8, 4, 8, 128), F32),
            DS((4,)), DS((2,)), DS((2, 3)), DS((XRING, 3)), DS((3, DEPTH)), DS((3, 2, RING)),
            DS((8,)), DS((8,)), DS, DS,
        ],
        compiler_params=pltpu.CompilerParams(collective_id=0, has_side_effects=True, vmem_limit_bytes=67043328),
    )(lab, mask, ht24, x_loc, w_in, w_out)


def solution(mesh):
    def local_step(x_loc, w_in, w_out, task_heads, lab_loc, mask_loc):
        by_class = task_heads.transpose(2, 0, 1)
        ht24 = jnp.pad(by_class, ((0, 0), (0, 2), (0, 0))).reshape(24, 512)
        ht24 = jnp.pad(ht24, ((0, 104), (0, 0)))
        alpha, g_in, g_out, _ = reduce_and_solve(lab_loc, mask_loc, ht24, x_loc, w_in, w_out)
        return alpha[0, :6], g_in.reshape(-1), g_out.reshape(-1)

    return jax.shard_map(local_step, mesh=mesh, in_specs=(P("data", None), P(), P(), P(), P(None, "data"), P(None, "data")), out_specs=(P(), P("data"), P("data")), check_vma=False)
```

```python
import functools

import jax
import jax.numpy as jnp
from jax import lax
from jax.experimental import pallas as pl
from jax.experimental.pallas import tpu as pltpu
from jax.sharding import PartitionSpec as P

SOLVER_STEPS = 20
T = 6
NT = (((1,), (1,)), ((), ()))
TILE = (8, 128)
MESH = pl.DeviceIdType.MESH
STRIDES = (32, 8, 2)
RING, DEPTH, XRING = 8, 4, 3
F32, BF16 = jnp.float32, jnp.bfloat16


def perm(order, z, y, x):
    return ((z, y, x), (y, x, z), (x, z, y))[order]


def kernel(lab_ref, mask_ref, ht24_ref, x_hbm, w1_hbm, w2_hbm,
           out_ref, gp_hbm,
           aT, xT, dz, w2, gp, q, hbig, code_ref, ht3_ref, other, inv, hb, xr, dbuf, ebuf, fbuf, r1, r2, r3, shard, gb, ar_s, ar_r,
           ld_sem, gp_sem, xs_sem, xr_sem, s_sem, r_sem, ars_sem, arr_sem, gs_sem, gr_sem):
    nchunk, nfb = 16, 8
    me = lax.axis_index("data")
    core = lax.rem(me, 2)
    coord = (lax.div(me, 32), lax.rem(lax.div(me, 8), 4), lax.rem(lax.div(me, 2), 4))
    partner = me + 1 - 2 * core

    def nb(dim, step):
        u = coord[dim]
        return (me + (lax.rem(u + step + 4, 4) - u) * STRIDES[dim],)

    def rel(dim, step):
        return lax.rem(coord[dim] + step + 4, 4)

    x_loads = [pltpu.make_async_copy(x_hbm.at[:, pl.ds(256 * i, 256)], q.at[i], ld_sem.at[i]) for i in range(2)]
    w1_load = pltpu.make_async_copy(w1_hbm, xT, ld_sem.at[2])
    w2_load = pltpu.make_async_copy(w2_hbm, w2, ld_sem.at[3])
    for c in x_loads + [w1_load, w2_load]:
        c.start()

    def gp_load(fb):
        return pltpu.make_async_copy(gp_hbm.at[fb], gp.at[lax.rem(fb, 2)], gp_sem.at[lax.rem(fb, 2)])

    def gp_store(fb):
        return pltpu.make_async_copy(gp.at[lax.rem(fb, 2)], gp_hbm.at[fb], gp_sem.at[lax.rem(fb, 2)])

    barrier = pltpu.get_barrier_semaphore()
    plane = 4 * coord[1] + coord[2]
    column = 2 * coord[0] + core
    plane_peers = [(nb(1, dy)[0] + nb(2, dx)[0] - me,) for dy in range(4) for dx in range(4) if dy or dx]
    column_peers = [(nb(0, dz_)[0] + dc * (partner - me),) for dz_ in range(4) for dc in range(2) if dz_ or dc]
    peers = plane_peers + column_peers
    for p in peers:
        pl.semaphore_signal(barrier, inc=1, device_id=p, device_id_type=MESH)
    pl.semaphore_wait(barrier, 22)

    def ar_start(base, stage, val):
        s = base + stage
        ar_s[s] = val
        for p in (plane_peers, column_peers)[stage]:
            pltpu.make_async_remote_copy(
                src_ref=ar_s.at[s], dst_ref=ar_r.at[s, (plane, column)[stage]], send_sem=ars_sem.at[s], recv_sem=arr_sem.at[s],
                device_id=p, device_id_type=MESH).start()

    def ar_finish(base, stage):
        s = base + stage
        n = (16, 8)[stage]
        rest = ar_r.at[s, pl.ds(0, n - 1)]
        pltpu.make_async_copy(rest, rest, arr_sem.at[s]).wait()
        pltpu.make_async_copy(rest, rest, ars_sem.at[s]).wait()
        part = [jnp.where((plane, column)[stage] == i, ar_s[s], ar_r[s, i]) for i in range(n)]
        while len(part) > 1:
            part = [a + b for a, b in zip(part[::2], part[1::2])]
        return part[0]

    def all_reduce(base, val):
        for stage in range(2):
            ar_start(base, stage, val)
            val = ar_finish(base, stage)
        return val

    code_ref[...] = jnp.full(code_ref.shape, -1.0, F32)
    code_ref[0:T, :] = jnp.where(mask_ref[...] > 0, lab_ref[...], -1).astype(F32)
    cnt = jnp.sum((code_ref[0:8, :] >= 0).astype(F32), axis=1, keepdims=True)
    ar_start(0, 0, jnp.broadcast_to(cnt, TILE))
    for c in x_loads + [w1_load]:
        c.wait()
    K0, K1 = 0.7978845608028654, 0.044715

    def hidden(fb, _):
        cols = pl.ds(pl.multiple_of(fb * 256, 256), 256)
        @pl.when(fb == 3)
        def _():
            ar_start(0, 1, ar_finish(0, 0))

        @pl.when(fb >= 2)
        def _():
            gp_store(fb - 2).wait()
        for i in range(4):
            rows = slice(512 * i, 512 * i + 512)
            p = (jnp.dot(q[0, rows, :], xT[0:256, cols], preferred_element_type=F32)
                 + jnp.dot(q[1, rows, :], xT[256:512, cols], preferred_element_type=F32))
            p2 = p * p
            th = jnp.tanh(p * (K0 + (K0 * K1) * p2))
            cdf = 0.5 + 0.5 * th
            wide = p * cdf
            act = wide.astype(BF16)
            gp[lax.rem(fb, 2), rows, :] = cdf + (wide * (1.0 - cdf)) * (2 * K0 + (6 * K0 * K1) * p2)
            dz[lax.div(fb, 2), rows, pl.ds(pl.multiple_of(lax.rem(fb, 2) * 256, 256), 256)] = act
            aT[pl.ds(fb * 8, 8), :, :, rows] = act.T.reshape(8, 2, 16, 512)

        @pl.when(fb < nfb - 2)
        def _():
            gp_store(fb).start()
        return 0
    lax.fori_loop(0, nfb, hidden, 0)

    inv_all = 1.0 / jnp.maximum(ar_finish(0, 1), 1.0)
    for t in range(T):
        inv[t] = jnp.broadcast_to(inv_all[t:t + 1, :], TILE)

    heads = ht24_ref[...].astype(F32)
    for c in range(3):
        ht3_ref[128 * c:128 * c + 128, :] = jnp.concatenate([heads[8 * c:8 * c + 8], jnp.zeros((120, 512), F32)], axis=0).astype(BF16)
    head_row = lax.rem(lax.broadcasted_iota(jnp.int32, (128, 512), 0), 8)
    for t in range(T):
        hbig[t] = jnp.where(head_row == t, heads, 0.0).astype(BF16)
    w2_load.wait()

    def tokens(i, _):
        rows = pl.ds(pl.multiple_of(i * 512, 512), 512)
        z = jnp.dot(dz[0, rows, :], w2[0:512, :], preferred_element_type=F32)
        for j in range(1, 4):
            z = z + jnp.dot(dz[j, rows, :], w2[512 * j:512 * j + 512, :], preferred_element_type=F32)
        x_t = jnp.concatenate([q[0, rows, :], q[1, rows, :]], axis=1)
        zb = (x_t.astype(F32) + z).astype(BF16)
        logits = lax.dot_general(zb, ht3_ref[...], NT, preferred_element_type=F32)
        ls = [logits[:, 128 * c:128 * c + 128] for c in range(3)]
        top = jnp.maximum(jnp.maximum(ls[0], ls[1]), ls[2])
        ex = [jnp.exp(v - top) for v in ls]
        den = ex[0] + ex[1] + ex[2]
        code = code_ref[:, rows].T
        errs = []
        for c in range(3):
            err = jnp.where(code >= 0, ex[c] / den - (code == c).astype(F32), 0.0)
            errs.append(err.astype(BF16).astype(F32))
        packed = (errs[0] + pltpu.roll(errs[1], 8, 1) + pltpu.roll(errs[2], 16, 1)).astype(BF16)
        for t in range(T):
            dz[t, rows, :] = jnp.dot(packed, hbig[t], preferred_element_type=F32).astype(BF16)
        xT[:, rows] = x_t.T
        return 0
    lax.fori_loop(0, 4, tokens, 0)

    srcs = (dbuf, ebuf, fbuf)
    recvs = (r1, r2, r3)

    def dims_of(p, t):
        return (t % 3 + p) % 3, (1 if t < 3 else -1)

    def drain_sends(p, d):
        ref = recvs[p].at[0]
        pltpu.make_async_copy(ref, ref, s_sem.at[p, d]).wait()

    def send(p, k, t, blk, kind, step, dim):
        slot, d = lax.rem(k, RING), lax.rem(k, DEPTH)
        pltpu.make_async_remote_copy(
            src_ref=srcs[p].at[d, t, blk], dst_ref=recvs[p].at[slot, kind, t],
            send_sem=s_sem.at[p, d], recv_sem=r_sem.at[p, 0 if kind == 0 else 1, slot],
            device_id=nb(dim, step), device_id_type=MESH).start()

    def open_phase(p, k, tasks=tuple(range(T))):
        for t in tasks:
            dim, sg = dims_of(p, t)
            send(p, k, t, rel(dim, 2), 0, jnp.where(k == nchunk - 1, 2, sg) if p == 2 else sg, dim)
        for t in tasks:
            dim, sg = dims_of(p, t)
            send(p, k, t, rel(dim, -sg), 1, -sg, dim)
        if p == 2:
            @pl.when(k == nchunk - 1)
            def _():
                for t in tasks:
                    dim, sg = dims_of(p, t)
                    send(p, k, t, rel(dim, sg), 2, sg, dim)

    def relay(p, k):
        slot, d = lax.rem(k, RING), lax.rem(k, DEPTH)
        ref = recvs[p].at[slot, 0]
        pltpu.make_async_copy(ref, ref, r_sem.at[p, 0, slot]).wait()
        for t in range(T):
            dim, sg = dims_of(p, t)
            v = rel(dim, sg)
            srcs[p][d, t, v] = srcs[p][d, t, v] + recvs[p][slot, 0, t]
        for t in range(T):
            dim, sg = dims_of(p, t)
            send(p, k, t, rel(dim, sg), 2, sg, dim)

    def close(p, k):
        slot, d = lax.rem(k, RING), lax.rem(k, DEPTH)
        ref = recvs[p].at[slot, pl.ds(1, 2)]
        pltpu.make_async_copy(ref, ref, r_sem.at[p, 1, slot]).wait()
        if p < 2:
            @pl.when(k >= DEPTH)
            def _():
                drain_sends(p + 1, d)
        else:
            @pl.when(k == nchunk - 1)
            def _():
                far = r3.at[slot, 0]
                pltpu.make_async_copy(far, far, r_sem.at[p, 0, slot]).wait()
                for t in range(T):
                    mine = coord[dims_of(p, t)[0]]
                    fbuf[d, t, mine] = fbuf[d, t, mine] + r3[slot, 0, t]
        for t in range(T):
            dim, _ = dims_of(p, t)
            out = srcs[p][d, t, coord[dim]] + recvs[p][slot, 1, t] + recvs[p][slot, 2, t]
            if p < 2:
                srcs[p + 1][d, t] = out
            else:
                shard[t, k] = out
        if p < 2:
            open_phase(p + 1, k)

    def pair_copy(k, third):
        hs, xs = lax.rem(k, 2), lax.rem(k, XRING)
        return pltpu.make_async_remote_copy(
            src_ref=hb.at[hs, 1 - core, pl.ds(2 * third, 2)], dst_ref=xr.at[xs, pl.ds(2 * third, 2)],
            send_sem=xs_sem.at[hs, third], recv_sem=xr_sem.at[xs, third],
            device_id=(partner,), device_id_type=MESH)

    def merge(pair, k):
        d, hs, xs = lax.rem(k, DEPTH), lax.rem(k, 2), lax.rem(k, XRING)
        pair_copy(k, pair).wait_recv()
        if pair == 0:
            @pl.when(k >= DEPTH)
            def _():
                drain_sends(0, d)
        for t in (2 * pair, 2 * pair + 1):
            for two in range(32):
                rows = slice(16 * two, 16 * two + 16)
                s = hb[hs, core, t, rows, :].astype(F32) + xr[xs, t, rows, :].astype(F32)
                for e in range(2):
                    i = 2 * two + e
                    a, b, c = perm(t % 3, i // 16, (i // 4) % 4, i % 4)
                    dbuf[d, t, a, b, c] = s[8 * e:8 * e + 8]
        open_phase(0, k, (2 * pair, 2 * pair + 1))

    def compute_out(k, third):
        j = lax.div(k, 2)
        h, cb = lax.div(j, 4), lax.rem(j, 4)
        hs, t = lax.rem(k, 2), 2 * third
        cols = pl.ds(pl.multiple_of(cb * 128, 128), 128)
        lhs = aT[:, h, :, :].reshape(1024, 2048)
        rhs = jnp.concatenate([dz[t, :, cols], dz[t + 1, :, cols]], axis=1)
        acc = jnp.dot(lhs, rhs, preferred_element_type=F32)
        for e in range(2):
            part = (acc[:, 128 * e:128 * e + 128] * inv[t + e][0:1, :]).reshape(64, 2, 8, 128)
            for c in range(2):
                hb[hs, c, t + e] = part[:, c].reshape(512, 128).astype(BF16)

    def compute_in(k, third):
        fb = lax.rem(lax.div(k, 2) + nfb - 2, nfb)
        hs, gs, t = lax.rem(k, 2), lax.rem(fb, 2), 2 * third

        @pl.when((third == 0) & (fb < nfb - 2))
        def _():
            gp_load(fb).wait()

        @pl.when((third == 0) & (fb != nfb - 2) & (fb != nfb - 3))
        def _():
            gp_load(lax.rem(fb + 1, nfb)).start()
        w_blk = w2[pl.ds(pl.multiple_of(fb * 256, 256), 256), :]
        for e in range(2):
            d_act = lax.dot_general(dz[t + e], w_blk, NT, preferred_element_type=F32)
            q[e] = (d_act * gp[gs]).astype(BF16)
        for e in range(2):
            acc = jnp.dot(xT[...], q[e], preferred_element_type=F32)
            row = inv[t + e][0:1, :]
            hb[hs, 0, t + e] = (acc[:, :128] * row).astype(BF16)
            hb[hs, 1, t + e] = (acc[:, 128:] * row).astype(BF16)

    def compute(k, third):
        @pl.when(k < nchunk)
        def _():
            @pl.when((third == 0) & (k >= 2))
            def _():
                for i in range(3):
                    pair_copy(k, i).wait_send()

            @pl.when(lax.rem(k, 2) == 0)
            def _():
                compute_out(k, third)

            @pl.when(lax.rem(k, 2) == 1)
            def _():
                compute_in(k, third)
            pair_copy(k, third).start()

    last = nchunk - 1

    def merge_all(k):
        for pair in range(3):
            merge(pair, k)

    def at(third, want, k, fn, lo=0, hi=nchunk):
        @pl.when((third == want) & (k >= lo) & (k < hi))
        def _():
            fn(k)

    def step(u, _):
        kk, third = lax.div(u, 3), lax.rem(u, 3)
        at(third, 0, kk - 3, functools.partial(relay, 0))
        at(third, 0, kk - 6, functools.partial(relay, 1))
        at(third, 0, kk - 9, functools.partial(relay, 2), hi=last)
        at(third, 1, kk - 1, merge_all, hi=last)
        at(third, 2, kk, functools.partial(merge, 0), lo=last)
        at(third, 0, kk - 1, functools.partial(merge, 1), lo=last)
        at(third, 1, kk - 1, functools.partial(merge, 2), lo=last)
        at(third, 1, kk - 4, functools.partial(close, 0))
        at(third, 1, kk - 7, functools.partial(close, 1))
        at(third, 1, kk - 10, functools.partial(close, 2))
        compute(kk, third)
        return 0
    lax.fori_loop(0, 3 * (nchunk + 10), step, 0)

    for i in range(DEPTH):
        for p in range(3):
            drain_sends(p, i)
    for k in (nchunk - 2, nchunk - 1):
        for third in range(3):
            pair_copy(k, third).wait_send()

    swap = pltpu.make_async_remote_copy(
        src_ref=shard, dst_ref=other, send_sem=gs_sem, recv_sem=gr_sem,
        device_id=(partner,), device_id_type=MESH)
    swap.start()

    pairs = [(t, s) for t in range(T) for s in range(t, T)]

    def gram_step(k, accs):
        rows = [shard[t, k] for t in range(T)]
        return tuple(acc + rows[t] * rows[s] for acc, (t, s) in zip(accs, pairs))
    accs = lax.fori_loop(0, nchunk, gram_step, tuple(jnp.zeros(TILE, F32) for _ in pairs))
    row_id = lax.broadcasted_iota(jnp.int32, TILE, 0)
    col_id = lax.broadcasted_iota(jnp.int32, TILE, 1)
    gram = jnp.zeros(TILE, F32)
    for acc, (t, s) in zip(accs, pairs):
        val = jnp.sum(jnp.sum(acc, axis=0, keepdims=True), axis=1, keepdims=True)
        hit = ((row_id == t) & (col_id == s)) | ((row_id == s) & (col_id == t))
        gram = jnp.where(hit, val, gram)
    gram = all_reduce(2, gram)

    def entry(t, s):
        return jnp.broadcast_to(gram[t:t + 1, s:s + 1], TILE)
    upper = {(t, s): entry(t, s) for t, s in pairs}
    scale = upper[0, 0]
    for t in range(1, T):
        scale = scale + upper[t, t]
    scale = scale / T

    def tree(v):
        return (v[0] + v[1]) + (v[2] + v[3]) + (v[4] + v[5])

    def solver(_, w):
        raised = []
        for t in range(T):
            pull = tree([upper[min(t, s), max(t, s)] * w[s] for s in range(T)])
            raised.append(w[t] * jnp.exp(-pull / scale))
        tot = tree(raised)
        return tuple(r / tot for r in raised)
    alphas = lax.fori_loop(0, SOLVER_STEPS, solver, tuple(jnp.full(TILE, 1.0 / T, F32) for _ in range(T)))
    packed = jnp.zeros(TILE, F32)
    for t in range(T):
        packed = jnp.where(col_id == t, alphas[t], packed)
    out_ref[128:136, :] = packed
    swap.wait()

    def combine(k, _):
        for ref, who in ((shard, core), (other, 1 - core)):
            gb[who, k] = tree([alphas[t] * ref[t, k] for t in range(T)])
        return 0
    lax.fori_loop(0, nchunk, combine, 0)
    for h in range(2):
        for fb in range(nfb):
            tile = gb[h, 2 * ((fb + 2) % nfb) + 1]
            rows = jnp.where(core == 0, tile[0:4], tile[4:8])
            for r in range(4):
                o = r * 2 * nfb + 2 * fb + h
                out_ref[o:o + 1, :] = rows[r:r + 1]
        for cb in range(4):
            tile = gb[h, 2 * (4 * core + cb)]
            for r in range(8):
                o = (8 * h + r) * 4 + cb
                out_ref[64 + o:65 + o, :] = tile[r:r + 1]


def reduce_and_solve(lab, mask, ht24, x_loc, w_in, w_out):
    any_spec = pl.BlockSpec(memory_space=pl.ANY)
    vm = pl.BlockSpec(memory_space=pltpu.VMEM)
    V = pltpu.VMEM
    DS = pltpu.SemaphoreType.DMA
    shapes = [(136, 128), (8, 2048, 256)]
    return pl.pallas_call(
        kernel,
        name="grads_rs",
        out_shape=[jax.ShapeDtypeStruct(s, F32) for s in shapes],
        in_specs=[vm] * 3 + [any_spec] * 3,
        out_specs=[vm, any_spec],
        scratch_shapes=[
            V((64, 2, 16, 2048), BF16), V((512, 2048), BF16), V((T, 2048, 512), BF16), V((2048, 512), BF16),
            V((2, 2048, 256), F32), V((2, 2048, 256), BF16), V((T, 128, 512), BF16),
            V((128, 2048), F32), V((384, 512), BF16), V((T, 16, *TILE), F32), V((T, *TILE), F32),
            V((2, 2, T, 512, 128), BF16), V((XRING, T, 512, 128), BF16),
            *[V((DEPTH, T) + (4,) * n + TILE, F32) for n in (3, 2, 1)],
            *[V((RING, 3, T) + (4,) * n + TILE, F32) for n in (2, 1, 0)],
            V((T, 16, *TILE), F32), V((2, 16, *TILE), F32), V((4, *TILE), F32), V((4, 16, *TILE), F32),
            DS((4,)), DS((2,)), DS((2, 3)), DS((XRING, 3)), DS((3, DEPTH)), DS((3, 2, RING)),
            DS((4,)), DS((4,)), DS, DS,
        ],
        compiler_params=pltpu.CompilerParams(collective_id=0, has_side_effects=True, vmem_limit_bytes=67043328),
    )(lab, mask, ht24, x_loc, w_in, w_out)


def solution(mesh):
    def local_step(x_loc, w_in, w_out, task_heads, lab_loc, mask_loc):
        by_class = task_heads.transpose(2, 0, 1)
        ht24 = jnp.pad(by_class, ((0, 0), (0, 2), (0, 0))).reshape(24, 512)
        ht24 = jnp.pad(ht24, ((0, 104), (0, 0)))
        out, _ = reduce_and_solve(lab_loc, mask_loc, ht24, x_loc, w_in, w_out)
        return out[128, :T], out[:64].reshape(-1), out[64:128].reshape(-1)

    return jax.shard_map(local_step, mesh=mesh, in_specs=(P("data", None), P(), P(), P(), P(None, "data"), P(None, "data")), out_specs=(P(), P("data"), P("data")), check_vma=False)
```
